512 devices in a mesh: seq: 128 (over x_lo, y, z), mp: 4 (over x_hi, core).
Axes of the slice: x: 4 (x_hi: 2, x_lo: 2; x = x_hi * 2 + x_lo), y: 4, z: 16, core: 2. Of those that a mesh axis runs over, the one named last changes fastest.
Arguments:
- incoming_image_patches: bfloat16 [1, 128, 128, 1152], P(None, 'seq', 'mp'), may hold values from -6 to 6
- initial_standardize_scaling: float32 [1152], replicated, may hold values from 0.1 to 1.9
- acceptance_matrix: bfloat16 [1152, 1024], P(None, 'mp'), may hold values from -0.1875 to 0.1875
- addressing_matrix: bfloat16 [1152, 1024], P(None, 'mp'), may hold values from -0.1875 to 0.1875
- content_matrix: bfloat16 [1152, 1024], P(None, 'mp'), may hold values from -0.1875 to 0.1875
- forgetting_lowdim_left_factor: bfloat16 [1152, 64], replicated, may hold values from -0.1875 to 0.1875
- forgetting_lowdim_right_factor: bfloat16 [64, 1024], P(None, 'mp'), may hold values from -1.5 to 1.5
- forgetting_baseline: float32 [1024], P('mp'), may hold values from -6 to 1
- self_token_reward: float32 [1024], P('mp'), may hold values from -3 to 3
- horizontal_cluster_scaling: float32 [1024], P('mp'), may hold values from 0.1 to 1.9
- vertical_cluster_scaling: float32 [1024], P('mp'), may hold values from 0.1 to 1.9
- temporal_mix_projection_matrix: bfloat16 [1024, 1152], P('mp'), may hold values from -0.1875 to 0.1875
- later_standardize_scaling: float32 [1152], replicated, may hold values from 0.1 to 1.9
- feature_mix_addressing_matrix: bfloat16 [1152, 4608], P('seq', 'mp'), may hold values from -0.1875 to 0.1875
- feature_mix_content_matrix: bfloat16 [4608, 1152], P('mp', 'seq'), may hold values from -0.09375 to 0.09375
Outputs:
- block_out: bfloat16 [1, 128, 128, 1152], P(None, 'seq', 'mp')
The draws below stay inside these ranges and needn't reach their ends.
All inputs are finite; a program needn't handle non-finite values.
Results may differ from the reference program's by a relative error of at most 0.017.
Values may be sent and summed in bfloat16 or wider, within the bound.
No kernel may reach another device: no remote copies, remote signals or barrier semaphores. Data moves between devices by JAX's collectives and lax.ppermute only.
A program may use at most 64 MiB of HBM per device.

```python
import jax
import jax.numpy as jnp
from jax import lax

MODEL_DIM = 1152
ATTENTION_SPLITS = 16
SUBSPACE_SIZE = 64
DECAY_RANK = 64
FF = 4608
IMGS = 1
HGT = 128
WID = 128
N_MP = 4


def steps_of(stream_key, dims, shards, smallest, top_value):
    def one(dim, shards_of):
        heights = jax.random.uniform(jax.random.fold_in(jax.random.fold_in(stream_key, 6), dim), (shards_of,), jnp.float32, smallest / len(shards), top_value / len(shards))
        return jnp.repeat(jnp.exp(heights), dims[dim] // shards_of).reshape((-1,) + (1,) * (len(dims) - dim - 1))

    level = one(*shards[0])
    for cut in shards[1:]:
        level = level * one(*cut)
    return level


def bell_draw(key, dims, deviation, limit, cuts=(), dtype=jnp.bfloat16):
    entries = jax.random.normal(key, dims, jnp.float32) * deviation
    if len(cuts) > 0:
        entries = steps_of(key, dims, cuts, -0.22, 0.18) * entries
    return jnp.clip(entries, min=-limit, max=limit).astype(dtype)


def setup_inputs(seed: int = 0) -> dict:
    key_of = jax.random.split(jax.random.key(seed), 16)
    incoming_image_patches = bell_draw(key_of[0], (IMGS, HGT, WID, MODEL_DIM), 1.0, 6.0, ((1, 128), (2, 4)))
    initial_standardize_scaling = jnp.clip(1.0 + 0.18 * jax.random.normal(key_of[1], (MODEL_DIM,), jnp.float32), 0.1, 1.9)
    acceptance_matrix = bell_draw(key_of[2], (MODEL_DIM, ATTENTION_SPLITS * SUBSPACE_SIZE), MODEL_DIM ** -0.5, 0.1875, ((1, 4),))
    addressing_matrix = bell_draw(key_of[3], (MODEL_DIM, ATTENTION_SPLITS * SUBSPACE_SIZE), MODEL_DIM ** -0.5, 0.1875, ((1, 4),))
    content_matrix = bell_draw(key_of[4], (MODEL_DIM, ATTENTION_SPLITS * SUBSPACE_SIZE), MODEL_DIM ** -0.5, 0.1875, ((1, 4),))
    forgetting_lowdim_left_factor = bell_draw(key_of[5], (MODEL_DIM, DECAY_RANK), MODEL_DIM ** -0.5, 0.1875)
    forgetting_lowdim_right_factor = bell_draw(key_of[6], (DECAY_RANK, ATTENTION_SPLITS * SUBSPACE_SIZE), 0.25, 1.5, ((1, 4),))
    forgetting_baseline = jnp.clip(-6.0 + 7.0 * jax.random.uniform(key_of[7], (ATTENTION_SPLITS * SUBSPACE_SIZE,), jnp.float32) ** steps_of(key_of[7], (ATTENTION_SPLITS * SUBSPACE_SIZE,), ((0, 4),), -0.2, 0.2), -6.0, 1.0)
    self_token_reward = bell_draw(key_of[8], (ATTENTION_SPLITS * SUBSPACE_SIZE,), 0.5, 3.0, ((0, 4),), jnp.float32)
    horizontal_cluster_scaling = jnp.clip(1.0 + 0.18 * jax.random.normal(key_of[9], (ATTENTION_SPLITS * SUBSPACE_SIZE,), jnp.float32), 0.1, 1.9)
    vertical_cluster_scaling = jnp.clip(1.0 + 0.18 * jax.random.normal(key_of[10], (ATTENTION_SPLITS * SUBSPACE_SIZE,), jnp.float32), 0.1, 1.9)
    temporal_mix_projection_matrix = bell_draw(key_of[11], (ATTENTION_SPLITS * SUBSPACE_SIZE, MODEL_DIM), (ATTENTION_SPLITS * SUBSPACE_SIZE) ** -0.5, 0.1875, ((0, 4),))
    later_standardize_scaling = jnp.clip(1.0 + 0.18 * jax.random.normal(key_of[12], (MODEL_DIM,), jnp.float32), 0.1, 1.9)
    feature_mix_addressing_matrix = bell_draw(key_of[13], (MODEL_DIM, FF), MODEL_DIM ** -0.5, 0.1875, ((0, 128), (1, 4)))
    feature_mix_content_matrix = bell_draw(key_of[14], (FF, MODEL_DIM), FF ** -0.5, 0.09375, ((0, 4), (1, 128)))
    return dict(incoming_image_patches=incoming_image_patches, initial_standardize_scaling=initial_standardize_scaling, acceptance_matrix=acceptance_matrix, addressing_matrix=addressing_matrix, content_matrix=content_matrix, forgetting_lowdim_left_factor=forgetting_lowdim_left_factor, forgetting_lowdim_right_factor=forgetting_lowdim_right_factor, forgetting_baseline=forgetting_baseline, self_token_reward=self_token_reward, horizontal_cluster_scaling=horizontal_cluster_scaling, vertical_cluster_scaling=vertical_cluster_scaling, temporal_mix_projection_matrix=temporal_mix_projection_matrix, later_standardize_scaling=later_standardize_scaling, feature_mix_addressing_matrix=feature_mix_addressing_matrix, feature_mix_content_matrix=feature_mix_content_matrix)


def layer_norm(inputs, gain):
    values = inputs.astype(jnp.float32)
    average = lax.optimization_barrier(jnp.mean(values, axis=-1, keepdims=True))
    centred = values - average
    spread = lax.optimization_barrier(jnp.mean(centred * centred, axis=-1, keepdims=True))
    return (centred * lax.rsqrt(spread + 1e-05) * gain).astype(jnp.bfloat16)

def heads_first(array, nheads):
    number, length, inner_width = array.shape
    shaped = array.astype(jnp.float32).reshape(number, length, nheads, inner_width // nheads)
    return shaped.transpose(0, 2, 1, 3)

def recurrence(recept_in, keying_in, decays_in, valued_in, boost_in, gain):
    number, length, inner_width = recept_in.shape
    nheads = inner_width // SUBSPACE_SIZE
    head_size = inner_width // nheads
    blocks = length // 16
    acceptance_horizontal_lines = heads_first(recept_in, nheads)
    addressing_horizontal_lines = heads_first(keying_in, nheads)
    decays = heads_first(decays_in, nheads)
    content_horizontal_lines = heads_first(valued_in, nheads)
    boost = boost_in.reshape(nheads, 1, head_size)
    running = jnp.cumsum(decays, axis=2)
    before = running - decays
    before_blocks = before.reshape(number, nheads, blocks, 16, head_size)
    anchor = before_blocks[:, :, :, :1, :]
    queries = acceptance_horizontal_lines.reshape(number, nheads, blocks, 16, head_size) * jnp.exp(before_blocks - anchor)
    places = jnp.arange(length)
    limits = (jnp.arange(blocks) + 1) * 16
    usable = places[None, :] < limits[:, None]
    exponent = anchor - running[:, :, None, :, :]
    exponent = jnp.where(usable[None, None, :, :, None], exponent, -10000.0)
    weighted = addressing_horizontal_lines[:, :, None, :, :] * jnp.exp(exponent)
    scores = jnp.einsum('nhbqc,nhbsc->nhbqs', queries, weighted, precision=lax.Precision.HIGHEST)
    query_places = places.reshape(blocks, 16)
    earlier = places[None, None, :] < query_places[:, :, None]
    scores = jnp.where(earlier[None, None], scores, 0.0)
    current = lax.optimization_barrier(jnp.sum(acceptance_horizontal_lines * boost * addressing_horizontal_lines, axis=-1))
    summed = jnp.einsum('nhbqs,nhsc->nhbqc', scores, content_horizontal_lines, precision=lax.Precision.HIGHEST)
    summed = summed.reshape(number, nheads, length, head_size) + current[..., None] * content_horizontal_lines
    average = lax.optimization_barrier(jnp.mean(summed, axis=-1, keepdims=True))
    centred = summed - average
    spread = lax.optimization_barrier(jnp.mean(centred * centred, axis=-1, keepdims=True))
    normed = (centred * lax.rsqrt(spread + 0.00064)).transpose(0, 2, 1, 3).reshape(number, length, inner_width)
    return (normed * gain).astype(jnp.bfloat16)

def single_strip_sweep(arrays, boost, gain):

    def single(items):
        return recurrence(items[0][None], items[1][None], items[2][None], items[3][None], boost, gain)[0]
    return lax.map(single, arrays)

def reference(incoming_image_patches, initial_standardize_scaling, acceptance_matrix, addressing_matrix, content_matrix, forgetting_lowdim_left_factor, forgetting_lowdim_right_factor, forgetting_baseline, self_token_reward, horizontal_cluster_scaling, vertical_cluster_scaling, temporal_mix_projection_matrix, later_standardize_scaling, feature_mix_addressing_matrix, feature_mix_content_matrix):
    inner_width = ATTENTION_SPLITS * SUBSPACE_SIZE
    xn1 = layer_norm(incoming_image_patches, initial_standardize_scaling).reshape(-1, MODEL_DIM)
    acceptance_horizontal_lines = jnp.dot(xn1, acceptance_matrix, preferred_element_type=jnp.float32).astype(jnp.bfloat16)
    addressing_horizontal_lines = jnp.dot(xn1, addressing_matrix, preferred_element_type=jnp.float32).astype(jnp.bfloat16)
    content_horizontal_lines = jnp.dot(xn1, content_matrix, preferred_element_type=jnp.float32).astype(jnp.bfloat16)
    latent = jnp.tanh(jnp.dot(xn1, forgetting_lowdim_left_factor, preferred_element_type=jnp.float32)).astype(jnp.bfloat16)
    forgetting_log_amount = (-0.7 * jax.nn.sigmoid(forgetting_baseline + jnp.dot(latent, forgetting_lowdim_right_factor, preferred_element_type=jnp.float32))).astype(jnp.bfloat16)

    def horizontal_sweep(array):
        return array.reshape(IMGS * HGT, WID, inner_width)

    def vertical_sweep(array):
        return array.reshape(IMGS, HGT, WID, inner_width).transpose(0, 2, 1, 3).reshape(IMGS * WID, HGT, inner_width)
    horizontal_recurrence_result = single_strip_sweep((horizontal_sweep(acceptance_horizontal_lines), horizontal_sweep(addressing_horizontal_lines), horizontal_sweep(forgetting_log_amount), horizontal_sweep(content_horizontal_lines)), self_token_reward, horizontal_cluster_scaling)
    vertical_recurrence_result = single_strip_sweep((vertical_sweep(acceptance_horizontal_lines), vertical_sweep(addressing_horizontal_lines), vertical_sweep(forgetting_log_amount), vertical_sweep(horizontal_recurrence_result)), self_token_reward, vertical_cluster_scaling)
    vertical_recurrence_result = vertical_recurrence_result.reshape(IMGS, WID, HGT, inner_width).transpose(0, 2, 1, 3).reshape(-1, inner_width)
    group = inner_width // N_MP
    attended = jnp.zeros((IMGS * HGT * WID, MODEL_DIM), jnp.float32)
    for index in range(N_MP):
        partial_value = jnp.dot(vertical_recurrence_result[:, index * group:(index + 1) * group], temporal_mix_projection_matrix[index * group:(index + 1) * group], preferred_element_type=jnp.float32)
        attended = attended + lax.optimization_barrier(partial_value.astype(jnp.bfloat16)).astype(jnp.float32)
    residual = (incoming_image_patches.reshape(-1, MODEL_DIM).astype(jnp.float32) + attended).astype(jnp.bfloat16)
    xn2 = layer_norm(residual, later_standardize_scaling)
    units = FF // N_MP
    mixed = jnp.zeros((IMGS * HGT * WID, MODEL_DIM), jnp.float32)
    for index in range(N_MP):
        hidden_pre = jnp.dot(xn2, feature_mix_addressing_matrix[:, index * units:(index + 1) * units], preferred_element_type=jnp.float32)
        positive = jnp.maximum(hidden_pre, 0.0)
        hidden = (positive * positive).astype(jnp.bfloat16)
        partial_value = jnp.dot(hidden, feature_mix_content_matrix[index * units:(index + 1) * units], preferred_element_type=jnp.float32)
        mixed = mixed + lax.optimization_barrier(partial_value.astype(jnp.bfloat16)).astype(jnp.float32)
    block_out = (residual.astype(jnp.float32) + mixed).astype(jnp.bfloat16)
    return block_out.reshape(IMGS, HGT, WID, MODEL_DIM)
```

```python
import jax
import jax.numpy as jnp
from jax import lax
from jax.sharding import Mesh
from jax.sharding import PartitionSpec as P

SUBSPACE_SIZE = 64
SEQ = ("x_lo", "y", "z")
MP = ("x_hi", "core")
PLANE = ("x_lo", "y")


def from_everyone(value, axis):
    copies = jnp.broadcast_to(value, (lax.axis_size(axis), *value.shape))
    return lax.all_to_all(copies, axis, split_axis=0, concat_axis=0, tiled=True)


def split_up(value, dim, size):
    lengths = value.shape
    pieces = value.reshape(*lengths[:dim], size, lengths[dim] // size, *lengths[dim + 1 :])
    return jnp.moveaxis(pieces, dim, 0)


def sent_and_summed(value, axis, dim):
    size = lax.axis_size(axis)
    pieces = lax.all_to_all(split_up(value, dim, size), axis, 0, 0, tiled=True)
    return jnp.sum(pieces.astype(jnp.float32), axis=0)


def layer_norm(inputs, gain):
    values = inputs.astype(jnp.float32)
    average = jnp.mean(values, axis=-1, keepdims=True)
    centred = values - average
    spread = jnp.mean(centred * centred, axis=-1, keepdims=True)
    return (centred * lax.rsqrt(spread + 1e-05) * gain).astype(jnp.bfloat16)


def heads_first(array, nheads):
    number, length, inner_width = array.shape
    shaped = array.astype(jnp.float32).reshape(number, length, nheads, inner_width // nheads)
    return shaped.transpose(0, 2, 1, 3)


def recurrence(recept_in, keying_in, decays_in, valued_in, boost_in, gain):
    number, length, inner_width = recept_in.shape
    nheads = inner_width // SUBSPACE_SIZE
    head_size = inner_width // nheads
    blocks = length // 16
    acceptance_horizontal_lines = heads_first(recept_in, nheads)
    addressing_horizontal_lines = heads_first(keying_in, nheads)
    decays = heads_first(decays_in, nheads)
    content_horizontal_lines = heads_first(valued_in, nheads)
    boost = boost_in.reshape(nheads, 1, head_size)
    running = jnp.cumsum(decays, axis=2)
    before = running - decays
    before_blocks = before.reshape(number, nheads, blocks, 16, head_size)
    anchor = before_blocks[:, :, :, :1, :]
    queries = acceptance_horizontal_lines.reshape(number, nheads, blocks, 16, head_size) * jnp.exp(
        before_blocks - anchor
    )
    places = jnp.arange(length)
    limits = (jnp.arange(blocks) + 1) * 16
    usable = places[None, :] < limits[:, None]
    exponent = anchor - running[:, :, None, :, :]
    exponent = jnp.where(usable[None, None, :, :, None], exponent, -10000.0)
    weighted = addressing_horizontal_lines[:, :, None, :, :] * jnp.exp(exponent)
    scores = jnp.einsum("nhbqc,nhbsc->nhbqs", queries, weighted, precision=lax.Precision.HIGHEST)
    query_places = places.reshape(blocks, 16)
    earlier = places[None, None, :] < query_places[:, :, None]
    scores = jnp.where(earlier[None, None], scores, 0.0)
    current = jnp.sum(acceptance_horizontal_lines * boost * addressing_horizontal_lines, axis=-1)
    summed = jnp.einsum(
        "nhbqs,nhsc->nhbqc", scores, content_horizontal_lines, precision=lax.Precision.HIGHEST
    )
    summed = (
        summed.reshape(number, nheads, length, head_size)
        + current[..., None] * content_horizontal_lines
    )
    average = jnp.mean(summed, axis=-1, keepdims=True)
    centred = summed - average
    spread = jnp.mean(centred * centred, axis=-1, keepdims=True)
    normed = (
        (centred * lax.rsqrt(spread + 0.00064))
        .transpose(0, 2, 1, 3)
        .reshape(number, length, inner_width)
    )
    return (normed * gain).astype(jnp.bfloat16)


def unit_order(planes, depth, width):
    stored = jnp.arange(planes * depth * width)
    z, rest = stored // (planes * width), stored % (planes * width)
    plane, row = rest // width, rest % width
    true_place = (plane * depth + z) * width + row
    return true_place


def shards(
    incoming_image_patches,
    initial_standardize_scaling,
    acceptance_matrix,
    addressing_matrix,
    content_matrix,
    forgetting_lowdim_left_factor,
    forgetting_lowdim_right_factor,
    forgetting_baseline,
    self_token_reward,
    horizontal_cluster_scaling,
    vertical_cluster_scaling,
    temporal_mix_projection_matrix,
    later_standardize_scaling,
    feature_mix_addressing_matrix,
    feature_mix_content_matrix,
):
    images, row_count, part_cols, model_width = incoming_image_patches.shape
    tokens = incoming_image_patches.reshape(part_cols, model_width)
    whole_rows = lax.all_gather(tokens, MP, axis=0, tiled=True)
    full_cols = whole_rows.shape[0]
    inner_width = acceptance_matrix.shape[1]

    planes, depth = lax.axis_size(PLANE), lax.axis_size("z")
    width = feature_mix_addressing_matrix.shape[0]
    pair = jnp.stack([feature_mix_addressing_matrix, feature_mix_content_matrix.T])
    plane_pair = from_everyone(pair, PLANE).reshape(planes, *pair.shape)
    plane_up = plane_pair[:, 0].reshape(planes * width, -1)
    plane_down = plane_pair[:, 1].reshape(planes * width, -1)
    full_up = lax.all_gather(plane_up, "z", axis=0, tiled=True)
    full_down = lax.all_gather(plane_down, "z", axis=0, tiled=True)

    xn1 = layer_norm(whole_rows, initial_standardize_scaling)
    recept = jnp.dot(xn1, acceptance_matrix, preferred_element_type=jnp.float32).astype(
        jnp.bfloat16
    )
    keying = jnp.dot(xn1, addressing_matrix, preferred_element_type=jnp.float32).astype(
        jnp.bfloat16
    )
    valued = jnp.dot(xn1, content_matrix, preferred_element_type=jnp.float32).astype(jnp.bfloat16)
    latent = jnp.tanh(
        jnp.dot(xn1, forgetting_lowdim_left_factor, preferred_element_type=jnp.float32)
    ).astype(jnp.bfloat16)
    decay = (
        -0.7
        * jax.nn.sigmoid(
            forgetting_baseline
            + jnp.dot(latent, forgetting_lowdim_right_factor, preferred_element_type=jnp.float32)
        )
    ).astype(jnp.bfloat16)
    row_out = recurrence(
        recept[None],
        keying[None],
        decay[None],
        valued[None],
        self_token_reward,
        horizontal_cluster_scaling,
    )[0]
    sent = jnp.stack([recept, keying, decay, row_out], axis=1)
    got = lax.all_to_all(
        sent.reshape(full_cols, 4 * inner_width // 128, 128),
        SEQ,
        split_axis=0,
        concat_axis=0,
        tiled=True,
    )
    height = got.shape[0]
    got = got.reshape(height, 4, inner_width)
    col_out = recurrence(
        got[None, :, 0],
        got[None, :, 1],
        got[None, :, 2],
        got[None, :, 3],
        self_token_reward,
        vertical_cluster_scaling,
    )[0]
    back = lax.all_to_all(
        col_out.reshape(height, inner_width // 128, 128),
        SEQ,
        split_axis=0,
        concat_axis=0,
        tiled=True,
    ).reshape(full_cols, inner_width)
    partial_value = jnp.dot(
        back, temporal_mix_projection_matrix, preferred_element_type=jnp.float32
    ).astype(jnp.bfloat16)
    attended = sent_and_summed(partial_value, MP, 0)
    residual = (tokens.astype(jnp.float32) + attended).astype(jnp.bfloat16)
    mix_input = layer_norm(residual, later_standardize_scaling)

    places = unit_order(planes, depth, width)
    moved = (jnp.arange(model_width)[:, None] == places[None, :]).astype(jnp.bfloat16)
    mix_input = jnp.dot(mix_input, moved, preferred_element_type=jnp.float32).astype(jnp.bfloat16)
    mix_all = lax.all_gather(mix_input, MP, axis=0, tiled=True)
    hidden_pre = jnp.dot(mix_all, full_up, preferred_element_type=jnp.float32)
    positive = jnp.maximum(hidden_pre, 0.0)
    hidden = (positive * positive).astype(jnp.bfloat16)
    downward = lax.dot_general(
        hidden, full_down, (((1,), (1,)), ((), ())), preferred_element_type=jnp.float32
    ).astype(jnp.bfloat16)
    downward = lax.dot_general(
        downward, moved, (((1,), (1,)), ((), ())), preferred_element_type=jnp.float32
    ).astype(jnp.bfloat16)
    mixed = sent_and_summed(downward, MP, 0)
    block_out = (residual.astype(jnp.float32) + mixed).astype(jnp.bfloat16)
    return block_out.reshape(images, row_count, part_cols, model_width)


def solution(mesh):
    torus = Mesh(mesh.devices.reshape(2, 4, 16, 2, 2), (*SEQ, *MP))
    return jax.shard_map(
        shards,
        mesh=torus,
        in_specs=(
            P(None, SEQ, MP, None),
            P(),
            P(None, MP),
            P(None, MP),
            P(None, MP),
            P(),
            P(None, MP),
            P(MP),
            P(MP),
            P(MP),
            P(MP),
            P(MP, None),
            P(),
            P(SEQ, MP),
            P(MP, SEQ),
        ),
        out_specs=P(None, SEQ, MP, None),
        check_vma=False,
    )
```

```python
import jax
import jax.numpy as jnp
from jax import lax
from jax.sharding import Mesh
from jax.sharding import PartitionSpec as P

SUBSPACE_SIZE = 64
SEQ = ("x_lo", "y", "z")
MP = ("x_hi", "core")
PLANE = ("x_lo", "y")


def from_everyone(value, axis):
    copies = jnp.broadcast_to(value, (lax.axis_size(axis), *value.shape))
    return lax.all_to_all(copies, axis, split_axis=0, concat_axis=0, tiled=True)


def split_up(value, dim, size):
    lengths = value.shape
    pieces = value.reshape(*lengths[:dim], size, lengths[dim] // size, *lengths[dim + 1 :])
    return jnp.moveaxis(pieces, dim, 0)


def sent_and_summed(value, axis, dim):
    size = lax.axis_size(axis)
    pieces = lax.all_to_all(split_up(value, dim, size), axis, 0, 0, tiled=True)
    return jnp.sum(pieces.astype(jnp.float32), axis=0)


def layer_norm(inputs, gain):
    values = inputs.astype(jnp.float32)
    average = jnp.mean(values, axis=-1, keepdims=True)
    centred = values - average
    spread = jnp.mean(centred * centred, axis=-1, keepdims=True)
    return (centred * lax.rsqrt(spread + 1e-05) * gain).astype(jnp.bfloat16)


def heads_first(array, nheads):
    number, length, inner_width = array.shape
    shaped = array.astype(jnp.float32).reshape(number, length, nheads, inner_width // nheads)
    return shaped.transpose(0, 2, 1, 3)


def recurrence(recept_in, keying_in, decays_in, valued_in, boost_in, gain):
    number, length, inner_width = recept_in.shape
    nheads = inner_width // SUBSPACE_SIZE
    head_size = inner_width // nheads
    blocks = length // 16
    acceptance_horizontal_lines = heads_first(recept_in, nheads)
    addressing_horizontal_lines = heads_first(keying_in, nheads)
    decays = heads_first(decays_in, nheads)
    content_horizontal_lines = heads_first(valued_in, nheads)
    boost = boost_in.reshape(nheads, 1, head_size)
    running = jnp.cumsum(decays, axis=2)
    before = running - decays
    before_blocks = before.reshape(number, nheads, blocks, 16, head_size)
    anchor = before_blocks[:, :, :, :1, :]
    queries = acceptance_horizontal_lines.reshape(number, nheads, blocks, 16, head_size) * jnp.exp(
        before_blocks - anchor
    )
    places = jnp.arange(length)
    limits = (jnp.arange(blocks) + 1) * 16
    usable = places[None, :] < limits[:, None]
    exponent = anchor - running[:, :, None, :, :]
    exponent = jnp.where(usable[None, None, :, :, None], exponent, -10000.0)
    weighted = addressing_horizontal_lines[:, :, None, :, :] * jnp.exp(exponent)
    scores = jnp.einsum("nhbqc,nhbsc->nhbqs", queries, weighted, precision=lax.Precision.HIGHEST)
    query_places = places.reshape(blocks, 16)
    earlier = places[None, None, :] < query_places[:, :, None]
    scores = jnp.where(earlier[None, None], scores, 0.0)
    current = jnp.sum(acceptance_horizontal_lines * boost * addressing_horizontal_lines, axis=-1)
    summed = jnp.einsum(
        "nhbqs,nhsc->nhbqc", scores, content_horizontal_lines, precision=lax.Precision.HIGHEST
    )
    summed = (
        summed.reshape(number, nheads, length, head_size)
        + current[..., None] * content_horizontal_lines
    )
    average = jnp.mean(summed, axis=-1, keepdims=True)
    centred = summed - average
    spread = jnp.mean(centred * centred, axis=-1, keepdims=True)
    normed = (
        (centred * lax.rsqrt(spread + 0.00064))
        .transpose(0, 2, 1, 3)
        .reshape(number, length, inner_width)
    )
    return (normed * gain).astype(jnp.bfloat16)


def unit_order(planes, depth, width):
    stored = jnp.arange(planes * depth * width)
    z, rest = stored // (planes * width), stored % (planes * width)
    plane, row = rest // width, rest % width
    true_place = (plane * depth + z) * width + row
    return true_place


def shards(
    incoming_image_patches,
    initial_standardize_scaling,
    acceptance_matrix,
    addressing_matrix,
    content_matrix,
    forgetting_lowdim_left_factor,
    forgetting_lowdim_right_factor,
    forgetting_baseline,
    self_token_reward,
    horizontal_cluster_scaling,
    vertical_cluster_scaling,
    temporal_mix_projection_matrix,
    later_standardize_scaling,
    feature_mix_addressing_matrix,
    feature_mix_content_matrix,
):
    images, row_count, part_cols, model_width = incoming_image_patches.shape
    tokens = incoming_image_patches.reshape(part_cols, model_width)
    whole_rows = lax.all_gather(tokens, MP, axis=0, tiled=True)
    full_cols = whole_rows.shape[0]
    inner_width = acceptance_matrix.shape[1]

    planes, depth = lax.axis_size(PLANE), lax.axis_size("z")
    width = feature_mix_addressing_matrix.shape[0]
    pair = jnp.stack([feature_mix_addressing_matrix, feature_mix_content_matrix.T])
    pair, whole_rows = lax.optimization_barrier((pair, whole_rows))
    plane_pair = from_everyone(pair, PLANE).reshape(planes, *pair.shape)
    plane_pair = jnp.swapaxes(plane_pair, 0, 1).reshape(2 * planes * width, -1)
    full_pair = lax.all_gather(plane_pair, "z", axis=0, tiled=True)
    full_pair = full_pair.reshape(depth, 2, planes * width, -1)
    full_up = full_pair[:, 0].reshape(model_width, -1)
    full_down = full_pair[:, 1].reshape(model_width, -1)

    xn1 = layer_norm(whole_rows, initial_standardize_scaling)
    recept = jnp.dot(xn1, acceptance_matrix, preferred_element_type=jnp.float32).astype(
        jnp.bfloat16
    )
    keying = jnp.dot(xn1, addressing_matrix, preferred_element_type=jnp.float32).astype(
        jnp.bfloat16
    )
    valued = jnp.dot(xn1, content_matrix, preferred_element_type=jnp.float32).astype(jnp.bfloat16)
    latent = jnp.tanh(
        jnp.dot(xn1, forgetting_lowdim_left_factor, preferred_element_type=jnp.float32)
    ).astype(jnp.bfloat16)
    decay = (
        -0.7
        * jax.nn.sigmoid(
            forgetting_baseline
            + jnp.dot(latent, forgetting_lowdim_right_factor, preferred_element_type=jnp.float32)
        )
    ).astype(jnp.bfloat16)
    row_out = recurrence(
        recept[None],
        keying[None],
        decay[None],
        valued[None],
        self_token_reward,
        horizontal_cluster_scaling,
    )[0]
    sent = jnp.stack([recept, keying, decay, row_out], axis=1)
    got = lax.all_to_all(
        sent.reshape(full_cols, 4 * inner_width // 128, 128),
        SEQ,
        split_axis=0,
        concat_axis=0,
        tiled=True,
    )
    height = got.shape[0]
    got = got.reshape(height, 4, inner_width)
    col_out = recurrence(
        got[None, :, 0],
        got[None, :, 1],
        got[None, :, 2],
        got[None, :, 3],
        self_token_reward,
        vertical_cluster_scaling,
    )[0]
    back = lax.all_to_all(
        col_out.reshape(height, inner_width // 128, 128),
        SEQ,
        split_axis=0,
        concat_axis=0,
        tiled=True,
    ).reshape(full_cols, inner_width)
    partial_value = jnp.dot(
        back, temporal_mix_projection_matrix, preferred_element_type=jnp.float32
    ).astype(jnp.bfloat16)
    attended = sent_and_summed(partial_value, MP, 0)
    residual = (tokens.astype(jnp.float32) + attended).astype(jnp.bfloat16)
    mix_input = layer_norm(residual, later_standardize_scaling)

    places = unit_order(planes, depth, width)
    moved = (jnp.arange(model_width)[:, None] == places[None, :]).astype(jnp.bfloat16)
    mix_input = jnp.dot(mix_input, moved, preferred_element_type=jnp.float32).astype(jnp.bfloat16)
    mix_all = lax.all_gather(mix_input, MP, axis=0, tiled=True)
    hidden_pre = jnp.dot(mix_all, full_up, preferred_element_type=jnp.float32)
    positive = jnp.maximum(hidden_pre, 0.0)
    hidden = (positive * positive).astype(jnp.bfloat16)
    downward = lax.dot_general(
        hidden, full_down, (((1,), (1,)), ((), ())), preferred_element_type=jnp.float32
    ).astype(jnp.bfloat16)
    downward = lax.dot_general(
        downward, moved, (((1,), (1,)), ((), ())), preferred_element_type=jnp.float32
    ).astype(jnp.bfloat16)
    mixed = sent_and_summed(downward, MP, 0)
    block_out = (residual.astype(jnp.float32) + mixed).astype(jnp.bfloat16)
    return block_out.reshape(images, row_count, part_cols, model_width)


def solution(mesh):
    torus = Mesh(mesh.devices.reshape(2, 4, 16, 2, 2), (*SEQ, *MP))
    return jax.shard_map(
        shards,
        mesh=torus,
        in_specs=(
            P(None, SEQ, MP, None),
            P(),
            P(None, MP),
            P(None, MP),
            P(None, MP),
            P(),
            P(None, MP),
            P(MP),
            P(MP),
            P(MP),
            P(MP),
            P(MP, None),
            P(),
            P(SEQ, MP),
            P(MP, SEQ),
        ),
        out_specs=P(None, SEQ, MP, None),
        check_vma=False,
    )
```

```python
import jax
import jax.numpy as jnp
from jax import lax
from jax.sharding import Mesh
from jax.sharding import PartitionSpec as P


SUBSPACE_SIZE = 64
SEQ = ("x_lo", "y", "z")
MP = ("x_hi", "core")
PLANE = ("x_lo", "y")


def from_everyone(value, axis):
    copies = jnp.broadcast_to(value, (lax.axis_size(axis), *value.shape))
    return lax.all_to_all(copies, axis, split_axis=0, concat_axis=0, tiled=True)


def split_up(value, dim, size):
    lengths = value.shape
    pieces = value.reshape(*lengths[:dim], size, lengths[dim] // size, *lengths[dim + 1 :])
    return jnp.moveaxis(pieces, dim, 0)


def sent_and_summed(value, axis, dim):
    size = lax.axis_size(axis)
    pieces = lax.all_to_all(split_up(value, dim, size), axis, 0, 0, tiled=True)
    return jnp.sum(pieces.astype(jnp.float32), axis=0)


def layer_norm(inputs, gain):
    values = inputs.astype(jnp.float32)
    average = jnp.mean(values, axis=-1, keepdims=True)
    centred = values - average
    spread = jnp.mean(centred * centred, axis=-1, keepdims=True)
    return (centred * lax.rsqrt(spread + 1e-05) * gain).astype(jnp.bfloat16)


def heads_first(array, nheads):
    number, length, inner_width = array.shape
    shaped = array.astype(jnp.float32).reshape(number, length, nheads, inner_width // nheads)
    return shaped.transpose(0, 2, 1, 3)


def recurrence(recept_in, keying_in, decays_in, valued_in, boost_in, gain):
    number, length, inner_width = recept_in.shape
    nheads = inner_width // SUBSPACE_SIZE
    head_size = inner_width // nheads
    blocks = length // 16
    acceptance_horizontal_lines = heads_first(recept_in, nheads)
    addressing_horizontal_lines = heads_first(keying_in, nheads)
    decays = heads_first(decays_in, nheads)
    content_horizontal_lines = heads_first(valued_in, nheads)
    boost = boost_in.reshape(nheads, 1, head_size)
    running = jnp.cumsum(decays, axis=2)
    before = running - decays
    before_blocks = before.reshape(number, nheads, blocks, 16, head_size)
    anchor = before_blocks[:, :, :, :1, :]
    queries = acceptance_horizontal_lines.reshape(number, nheads, blocks, 16, head_size) * jnp.exp(
        before_blocks - anchor
    )
    places = jnp.arange(length)
    limits = (jnp.arange(blocks) + 1) * 16
    usable = places[None, :] < limits[:, None]
    exponent = anchor - running[:, :, None, :, :]
    exponent = jnp.where(usable[None, None, :, :, None], exponent, -10000.0)
    weighted = addressing_horizontal_lines[:, :, None, :, :] * jnp.exp(exponent)
    scores = jnp.einsum("nhbqc,nhbsc->nhbqs", queries, weighted, precision=lax.Precision.HIGHEST)
    query_places = places.reshape(blocks, 16)
    earlier = places[None, None, :] < query_places[:, :, None]
    scores = jnp.where(earlier[None, None], scores, 0.0)
    current = jnp.sum(acceptance_horizontal_lines * boost * addressing_horizontal_lines, axis=-1)
    summed = jnp.einsum(
        "nhbqs,nhsc->nhbqc", scores, content_horizontal_lines, precision=lax.Precision.HIGHEST
    )
    summed = (
        summed.reshape(number, nheads, length, head_size)
        + current[..., None] * content_horizontal_lines
    )
    average = jnp.mean(summed, axis=-1, keepdims=True)
    centred = summed - average
    spread = jnp.mean(centred * centred, axis=-1, keepdims=True)
    normed = (
        (centred * lax.rsqrt(spread + 0.00064))
        .transpose(0, 2, 1, 3)
        .reshape(number, length, inner_width)
    )
    return (normed * gain).astype(jnp.bfloat16)


def unit_order(planes, depth, width):
    stored = jnp.arange(planes * depth * width)
    z, rest = stored // (planes * width), stored % (planes * width)
    plane, row = rest // width, rest % width
    true_place = (plane * depth + z) * width + row
    return true_place


def shards(
    incoming_image_patches,
    initial_standardize_scaling,
    acceptance_matrix,
    addressing_matrix,
    content_matrix,
    forgetting_lowdim_left_factor,
    forgetting_lowdim_right_factor,
    forgetting_baseline,
    self_token_reward,
    horizontal_cluster_scaling,
    vertical_cluster_scaling,
    temporal_mix_projection_matrix,
    later_standardize_scaling,
    feature_mix_addressing_matrix,
    feature_mix_content_matrix,
):
    images, row_count, part_cols, model_width = incoming_image_patches.shape
    tokens = incoming_image_patches.reshape(part_cols, model_width)
    whole_rows = lax.all_gather(tokens, MP, axis=0, tiled=True)
    full_cols = whole_rows.shape[0]
    inner_width = acceptance_matrix.shape[1]

    planes, depth = lax.axis_size(PLANE), lax.axis_size("z")
    width = feature_mix_addressing_matrix.shape[0]
    pair = jnp.stack([feature_mix_addressing_matrix, feature_mix_content_matrix.T])
    plane_pair = from_everyone(pair, PLANE)
    plane_pair = plane_pair.reshape(planes, *pair.shape)
    plane_pair = jnp.swapaxes(plane_pair, 0, 1).reshape(2 * planes * width, -1)
    full_pair = lax.all_gather(plane_pair, "z", axis=0, tiled=True)
    full_pair = full_pair.reshape(depth, 2, planes * width, -1)
    full_up = full_pair[:, 0].reshape(model_width, -1)
    full_down = full_pair[:, 1].reshape(model_width, -1)

    xn1 = layer_norm(whole_rows, initial_standardize_scaling)
    recept = jnp.dot(xn1, acceptance_matrix, preferred_element_type=jnp.float32).astype(
        jnp.bfloat16
    )
    keying = jnp.dot(xn1, addressing_matrix, preferred_element_type=jnp.float32).astype(
        jnp.bfloat16
    )
    valued = jnp.dot(xn1, content_matrix, preferred_element_type=jnp.float32).astype(jnp.bfloat16)
    latent = jnp.tanh(
        jnp.dot(xn1, forgetting_lowdim_left_factor, preferred_element_type=jnp.float32)
    ).astype(jnp.bfloat16)
    decay = (
        -0.7
        * jax.nn.sigmoid(
            forgetting_baseline
            + jnp.dot(latent, forgetting_lowdim_right_factor, preferred_element_type=jnp.float32)
        )
    ).astype(jnp.bfloat16)
    row_out = recurrence(
        recept[None],
        keying[None],
        decay[None],
        valued[None],
        self_token_reward,
        horizontal_cluster_scaling,
    )[0]
    sent = jnp.stack([recept, keying, decay, row_out], axis=1)
    sent = sent.reshape(full_cols, 4 * inner_width // 128, 128)
    sent, own_projection = lax.optimization_barrier((sent, temporal_mix_projection_matrix))
    got = lax.all_to_all(sent, SEQ, split_axis=0, concat_axis=0, tiled=True)
    projection = [own_projection]
    for k in range(1, 4):
        projection.append(lax.ppermute(own_projection, MP, [(i, i ^ k) for i in range(4)]))
    height = got.shape[0]
    got = got.reshape(height, 4, inner_width)
    col_out = recurrence(
        got[None, :, 0],
        got[None, :, 1],
        got[None, :, 2],
        got[None, :, 3],
        self_token_reward,
        vertical_cluster_scaling,
    )[0]
    back = lax.all_to_all(
        col_out.reshape(height, inner_width // 128, 128),
        SEQ,
        split_axis=0,
        concat_axis=0,
        tiled=True,
    ).reshape(full_cols, inner_width)
    group = lax.axis_index(MP)
    groups = lax.all_gather(back, MP, axis=0, tiled=False)
    attended = jnp.zeros((full_cols, model_width), jnp.float32)
    for k in range(4):
        one = lax.dynamic_index_in_dim(groups, group ^ k, 0, keepdims=False)
        attended = attended + jnp.dot(one, projection[k], preferred_element_type=jnp.float32)
    residual_all = (whole_rows.astype(jnp.float32) + attended).astype(jnp.bfloat16)
    residual = lax.dynamic_slice_in_dim(residual_all, group * part_cols, part_cols, 0)
    mix_input = layer_norm(residual_all, later_standardize_scaling)

    places = unit_order(planes, depth, width)
    moved = (jnp.arange(model_width)[:, None] == places[None, :]).astype(jnp.bfloat16)
    mix_input = jnp.dot(mix_input, moved, preferred_element_type=jnp.float32).astype(jnp.bfloat16)
    hidden_pre = jnp.dot(mix_input, full_up, preferred_element_type=jnp.float32)
    positive = jnp.maximum(hidden_pre, 0.0)
    hidden = (positive * positive).astype(jnp.bfloat16)
    downward = lax.dot_general(
        hidden, full_down, (((1,), (1,)), ((), ())), preferred_element_type=jnp.float32
    ).astype(jnp.bfloat16)
    downward = lax.dot_general(
        downward, moved, (((1,), (1,)), ((), ())), preferred_element_type=jnp.float32
    ).astype(jnp.bfloat16)
    mixed = sent_and_summed(downward, MP, 0)
    block_out = (residual.astype(jnp.float32) + mixed).astype(jnp.bfloat16)
    return block_out.reshape(images, row_count, part_cols, model_width)


def solution(mesh):
    torus = Mesh(mesh.devices.reshape(2, 4, 16, 2, 2), (*SEQ, *MP))
    return jax.shard_map(
        shards,
        mesh=torus,
        in_specs=(
            P(None, SEQ, MP, None),
            P(),
            P(None, MP),
            P(None, MP),
            P(None, MP),
            P(),
            P(None, MP),
            P(MP),
            P(MP),
            P(MP),
            P(MP),
            P(MP, None),
            P(),
            P(SEQ, MP),
            P(MP, SEQ),
        ),
        out_specs=P(None, SEQ, MP, None),
        check_vma=False,
    )
```

```python
import jax
import jax.numpy as jnp
from jax import lax
from jax.sharding import Mesh
from jax.sharding import PartitionSpec as P


SUBSPACE_SIZE = 64
SEQ = ("x_lo", "y", "z")
MP = ("x_hi", "core")
MIX = ("x_lo", "x_hi", "core")


def from_everyone(value, axis):
    copies = jnp.broadcast_to(value, (lax.axis_size(axis), *value.shape))
    return lax.all_to_all(copies, axis, split_axis=0, concat_axis=0, tiled=True)


def split_up(value, dim, size):
    lengths = value.shape
    pieces = value.reshape(*lengths[:dim], size, lengths[dim] // size, *lengths[dim + 1 :])
    return jnp.moveaxis(pieces, dim, 0)


def sent_and_summed(value, axis, dim):
    size = lax.axis_size(axis)
    pieces = lax.all_to_all(split_up(value, dim, size), axis, 0, 0, tiled=True)
    return jnp.sum(pieces.astype(jnp.float32), axis=0)


def layer_norm(inputs, gain):
    values = inputs.astype(jnp.float32)
    average = jnp.mean(values, axis=-1, keepdims=True)
    centred = values - average
    spread = jnp.mean(centred * centred, axis=-1, keepdims=True)
    return (centred * lax.rsqrt(spread + 1e-05) * gain).astype(jnp.bfloat16)


def heads_first(array, nheads):
    number, length, inner_width = array.shape
    shaped = array.astype(jnp.float32).reshape(number, length, nheads, inner_width // nheads)
    return shaped.transpose(0, 2, 1, 3)


def recurrence(recept_in, keying_in, decays_in, valued_in, boost_in, gain):
    number, length, inner_width = recept_in.shape
    nheads = inner_width // SUBSPACE_SIZE
    head_size = inner_width // nheads
    blocks = length // 16
    acceptance_horizontal_lines = heads_first(recept_in, nheads)
    addressing_horizontal_lines = heads_first(keying_in, nheads)
    decays = heads_first(decays_in, nheads)
    content_horizontal_lines = heads_first(valued_in, nheads)
    boost = boost_in.reshape(nheads, 1, head_size)
    running = jnp.cumsum(decays, axis=2)
    before = running - decays
    before_blocks = before.reshape(number, nheads, blocks, 16, head_size)
    anchor = before_blocks[:, :, :, :1, :]
    queries = acceptance_horizontal_lines.reshape(number, nheads, blocks, 16, head_size) * jnp.exp(
        before_blocks - anchor
    )
    places = jnp.arange(length)
    limits = (jnp.arange(blocks) + 1) * 16
    usable = places[None, :] < limits[:, None]
    exponent = anchor - running[:, :, None, :, :]
    exponent = jnp.where(usable[None, None, :, :, None], exponent, -10000.0)
    weighted = addressing_horizontal_lines[:, :, None, :, :] * jnp.exp(exponent)
    scores = jnp.einsum("nhbqc,nhbsc->nhbqs", queries, weighted, precision=lax.Precision.HIGHEST)
    query_places = places.reshape(blocks, 16)
    earlier = places[None, None, :] < query_places[:, :, None]
    scores = jnp.where(earlier[None, None], scores, 0.0)
    current = jnp.sum(acceptance_horizontal_lines * boost * addressing_horizontal_lines, axis=-1)
    summed = jnp.einsum(
        "nhbqs,nhsc->nhbqc", scores, content_horizontal_lines, precision=lax.Precision.HIGHEST
    )
    summed = (
        summed.reshape(number, nheads, length, head_size)
        + current[..., None] * content_horizontal_lines
    )
    average = jnp.mean(summed, axis=-1, keepdims=True)
    centred = summed - average
    spread = jnp.mean(centred * centred, axis=-1, keepdims=True)
    normed = (
        (centred * lax.rsqrt(spread + 0.00064))
        .transpose(0, 2, 1, 3)
        .reshape(number, length, inner_width)
    )
    return (normed * gain).astype(jnp.bfloat16)


def unit_order(depth, width):
    ring = lax.axis_size("y")
    stored = jnp.arange(2 * ring * depth * width)
    turn, rest = stored // (2 * depth * width), stored % (2 * depth * width)
    z, rest = rest // (2 * width), rest % (2 * width)
    x = rest // width
    y = (turn + lax.axis_index("y")) % ring
    return ((x * ring + y) * depth + z) * width + rest % width


def shards(
    incoming_image_patches,
    initial_standardize_scaling,
    acceptance_matrix,
    addressing_matrix,
    content_matrix,
    forgetting_lowdim_left_factor,
    forgetting_lowdim_right_factor,
    forgetting_baseline,
    self_token_reward,
    horizontal_cluster_scaling,
    vertical_cluster_scaling,
    temporal_mix_projection_matrix,
    later_standardize_scaling,
    feature_mix_addressing_matrix,
    feature_mix_content_matrix,
):
    images, row_count, part_cols, model_width = incoming_image_patches.shape
    tokens = incoming_image_patches.reshape(part_cols, model_width)
    whole_rows = lax.all_gather(tokens, MP, axis=0, tiled=True)
    full_cols = whole_rows.shape[0]
    inner_width = acceptance_matrix.shape[1]

    depth = lax.axis_size("z")
    width, units = feature_mix_addressing_matrix.shape
    first_half = lax.axis_index("x_lo") == 0
    halves = [
        jnp.concatenate(
            [
                feature_mix_addressing_matrix[:, start : start + units // 2],
                feature_mix_content_matrix.T[:, start : start + units // 2],
            ],
            axis=1,
        )
        for start in (0, units // 2)
    ]
    kept = jnp.where(first_half, halves[0], halves[1])
    given = jnp.where(first_half, halves[1], halves[0])
    received = lax.ppermute(given, "x_lo", [(0, 1), (1, 0)])
    pair = jnp.concatenate(
        [jnp.where(first_half, kept, received), jnp.where(first_half, received, kept)], axis=0
    )

    xn1 = layer_norm(whole_rows, initial_standardize_scaling)
    recept = jnp.dot(xn1, acceptance_matrix, preferred_element_type=jnp.float32).astype(
        jnp.bfloat16
    )
    keying = jnp.dot(xn1, addressing_matrix, preferred_element_type=jnp.float32).astype(
        jnp.bfloat16
    )
    valued = jnp.dot(xn1, content_matrix, preferred_element_type=jnp.float32).astype(jnp.bfloat16)
    latent = jnp.tanh(
        jnp.dot(xn1, forgetting_lowdim_left_factor, preferred_element_type=jnp.float32)
    ).astype(jnp.bfloat16)
    decay = (
        -0.7
        * jax.nn.sigmoid(
            forgetting_baseline
            + jnp.dot(latent, forgetting_lowdim_right_factor, preferred_element_type=jnp.float32)
        )
    ).astype(jnp.bfloat16)
    row_out = recurrence(
        recept[None],
        keying[None],
        decay[None],
        valued[None],
        self_token_reward,
        horizontal_cluster_scaling,
    )[0]
    sent = jnp.stack([recept, keying, decay, row_out], axis=1)
    sent = sent.reshape(full_cols, 4 * inner_width // 128, 128)
    sent, pair = lax.optimization_barrier((sent, pair))
    got = lax.all_to_all(sent, SEQ, split_axis=0, concat_axis=0, tiled=True)
    ring_pair = lax.all_gather(pair, "z", axis=0, tiled=True)
    height = got.shape[0]
    got = got.reshape(height, 4, inner_width)
    col_out = recurrence(
        got[None, :, 0],
        got[None, :, 1],
        got[None, :, 2],
        got[None, :, 3],
        self_token_reward,
        vertical_cluster_scaling,
    )[0]
    col_sent = col_out.reshape(height, inner_width // 128, 128)
    col_sent, ring_pair = lax.optimization_barrier((col_sent, ring_pair))
    back = lax.all_to_all(col_sent, SEQ, split_axis=0, concat_axis=0, tiled=True)
    back = back.reshape(full_cols, inner_width)
    pieces = [ring_pair]
    for k in range(1, 4):
        pieces.append(lax.ppermute(ring_pair, "y", [(i, (i - k) % 4) for i in range(4)]))
    partial_value = jnp.dot(
        back, temporal_mix_projection_matrix, preferred_element_type=jnp.float32
    ).astype(jnp.bfloat16)
    attended = sent_and_summed(partial_value, MP, 0)
    residual = (tokens.astype(jnp.float32) + attended).astype(jnp.bfloat16)
    mix_input = layer_norm(residual, later_standardize_scaling)

    places = unit_order(depth, width)
    moved = (jnp.arange(model_width)[:, None] == places[None, :]).astype(jnp.bfloat16)
    mix_input = jnp.dot(mix_input, moved, preferred_element_type=jnp.float32).astype(jnp.bfloat16)
    mix_all = from_everyone(mix_input, MIX).reshape(-1, model_width)
    weights = jnp.concatenate(pieces, axis=0)
    hidden_pre = jnp.dot(mix_all, weights, preferred_element_type=jnp.float32)
    positive = jnp.maximum(hidden_pre[:, : units // 2], 0.0)
    hidden = (positive * positive).astype(jnp.bfloat16)
    hidden = jnp.pad(hidden, ((0, 0), (units // 2, 0)))
    downward = lax.dot_general(
        hidden, weights, (((1,), (1,)), ((), ())), preferred_element_type=jnp.float32
    ).astype(jnp.bfloat16)
    downward = lax.dot_general(
        downward, moved, (((1,), (1,)), ((), ())), preferred_element_type=jnp.float32
    ).astype(jnp.bfloat16)
    mixed = sent_and_summed(downward, MIX, 0)
    block_out = (residual.astype(jnp.float32) + mixed).astype(jnp.bfloat16)
    return block_out.reshape(images, row_count, part_cols, model_width)


def solution(mesh):
    torus = Mesh(mesh.devices.reshape(2, 4, 16, 2, 2), (*SEQ, *MP))
    return jax.shard_map(
        shards,
        mesh=torus,
        in_specs=(
            P(None, SEQ, MP, None),
            P(),
            P(None, MP),
            P(None, MP),
            P(None, MP),
            P(),
            P(None, MP),
            P(MP),
            P(MP),
            P(MP),
            P(MP),
            P(MP, None),
            P(),
            P(SEQ, MP),
            P(MP, SEQ),
        ),
        out_specs=P(None, SEQ, MP, None),
        check_vma=False,
    )
```

```python
import jax
import jax.numpy as jnp
from jax import lax
from jax.sharding import Mesh
from jax.sharding import PartitionSpec as P


SUBSPACE_SIZE = 64
SEQ = ("x_lo", "y", "z")
MP = ("x_hi", "core")
PLANE = ("x_lo", "y")
MIX = ("x_lo", "x_hi", "core")


def from_everyone(value, axis):
    copies = jnp.broadcast_to(value, (lax.axis_size(axis), *value.shape))
    return lax.all_to_all(copies, axis, split_axis=0, concat_axis=0, tiled=True)


def split_up(value, dim, size):
    lengths = value.shape
    pieces = value.reshape(*lengths[:dim], size, lengths[dim] // size, *lengths[dim + 1 :])
    return jnp.moveaxis(pieces, dim, 0)


def sent_and_summed(value, axis, dim):
    size = lax.axis_size(axis)
    pieces = lax.all_to_all(split_up(value, dim, size), axis, 0, 0, tiled=True)
    return jnp.sum(pieces.astype(jnp.float32), axis=0)


def layer_norm(inputs, gain):
    values = inputs.astype(jnp.float32)
    average = jnp.mean(values, axis=-1, keepdims=True)
    centred = values - average
    spread = jnp.mean(centred * centred, axis=-1, keepdims=True)
    return (centred * lax.rsqrt(spread + 1e-05) * gain).astype(jnp.bfloat16)


def heads_first(array, nheads):
    number, length, inner_width = array.shape
    shaped = array.astype(jnp.float32).reshape(number, length, nheads, inner_width // nheads)
    return shaped.transpose(0, 2, 1, 3)


def recurrence(recept_in, keying_in, decays_in, valued_in, boost_in, gain):
    number, length, inner_width = recept_in.shape
    nheads = inner_width // SUBSPACE_SIZE
    head_size = inner_width // nheads
    blocks = length // 16
    acceptance_horizontal_lines = heads_first(recept_in, nheads)
    addressing_horizontal_lines = heads_first(keying_in, nheads)
    decays = heads_first(decays_in, nheads)
    content_horizontal_lines = heads_first(valued_in, nheads)
    boost = boost_in.reshape(nheads, 1, head_size)
    running = jnp.cumsum(decays, axis=2)
    before = running - decays
    before_blocks = before.reshape(number, nheads, blocks, 16, head_size)
    anchor = before_blocks[:, :, :, :1, :]
    queries = acceptance_horizontal_lines.reshape(number, nheads, blocks, 16, head_size) * jnp.exp(
        before_blocks - anchor
    )
    places = jnp.arange(length)
    limits = (jnp.arange(blocks) + 1) * 16
    usable = places[None, :] < limits[:, None]
    exponent = anchor - running[:, :, None, :, :]
    exponent = jnp.where(usable[None, None, :, :, None], exponent, -10000.0)
    weighted = addressing_horizontal_lines[:, :, None, :, :] * jnp.exp(exponent)
    scores = jnp.einsum("nhbqc,nhbsc->nhbqs", queries, weighted, precision=lax.Precision.HIGHEST)
    query_places = places.reshape(blocks, 16)
    earlier = places[None, None, :] < query_places[:, :, None]
    scores = jnp.where(earlier[None, None], scores, 0.0)
    current = jnp.sum(acceptance_horizontal_lines * boost * addressing_horizontal_lines, axis=-1)
    summed = jnp.einsum(
        "nhbqs,nhsc->nhbqc", scores, content_horizontal_lines, precision=lax.Precision.HIGHEST
    )
    summed = (
        summed.reshape(number, nheads, length, head_size)
        + current[..., None] * content_horizontal_lines
    )
    average = jnp.mean(summed, axis=-1, keepdims=True)
    centred = summed - average
    spread = jnp.mean(centred * centred, axis=-1, keepdims=True)
    normed = (
        (centred * lax.rsqrt(spread + 0.00064))
        .transpose(0, 2, 1, 3)
        .reshape(number, length, inner_width)
    )
    return (normed * gain).astype(jnp.bfloat16)


def unit_order(planes, depth, width):
    stored = jnp.arange(planes * depth * width)
    z, rest = stored // (planes * width), stored % (planes * width)
    return ((rest // width) * depth + z) * width + rest % width


def shards(
    incoming_image_patches,
    initial_standardize_scaling,
    acceptance_matrix,
    addressing_matrix,
    content_matrix,
    forgetting_lowdim_left_factor,
    forgetting_lowdim_right_factor,
    forgetting_baseline,
    self_token_reward,
    horizontal_cluster_scaling,
    vertical_cluster_scaling,
    temporal_mix_projection_matrix,
    later_standardize_scaling,
    feature_mix_addressing_matrix,
    feature_mix_content_matrix,
):
    images, row_count, part_cols, model_width = incoming_image_patches.shape
    tokens = incoming_image_patches.reshape(part_cols, model_width)
    whole_rows = lax.all_gather(tokens, MP, axis=0, tiled=True)
    full_cols = whole_rows.shape[0]
    inner_width = acceptance_matrix.shape[1]

    planes, depth, ring = lax.axis_size(PLANE), lax.axis_size("z"), lax.axis_size("y")
    width, units = feature_mix_addressing_matrix.shape
    halves = [
        jnp.concatenate(
            [
                feature_mix_addressing_matrix[:, start : start + units // 2],
                feature_mix_content_matrix.T[:, start : start + units // 2],
            ],
            axis=1,
        )
        for start in (0, units // 2)
    ]
    shares = jnp.broadcast_to(jnp.stack(halves)[:, None], (2, ring, width, units))
    plane = lax.all_to_all(shares.reshape(planes, width, units), PLANE, 0, 0, tiled=True)
    plane, whole_rows = lax.optimization_barrier(
        (plane.reshape(planes * width, units), whole_rows)
    )
    weights = lax.all_gather(plane, "z", axis=0, tiled=True)

    xn1 = layer_norm(whole_rows, initial_standardize_scaling)
    recept = jnp.dot(xn1, acceptance_matrix, preferred_element_type=jnp.float32).astype(
        jnp.bfloat16
    )
    keying = jnp.dot(xn1, addressing_matrix, preferred_element_type=jnp.float32).astype(
        jnp.bfloat16
    )
    valued = jnp.dot(xn1, content_matrix, preferred_element_type=jnp.float32).astype(jnp.bfloat16)
    latent = jnp.tanh(
        jnp.dot(xn1, forgetting_lowdim_left_factor, preferred_element_type=jnp.float32)
    ).astype(jnp.bfloat16)
    decay = (
        -0.7
        * jax.nn.sigmoid(
            forgetting_baseline
            + jnp.dot(latent, forgetting_lowdim_right_factor, preferred_element_type=jnp.float32)
        )
    ).astype(jnp.bfloat16)
    row_out = recurrence(
        recept[None],
        keying[None],
        decay[None],
        valued[None],
        self_token_reward,
        horizontal_cluster_scaling,
    )[0]
    sent = jnp.stack([recept, keying, decay, row_out], axis=1)
    sent = sent.reshape(full_cols, 4 * inner_width // 128, 128)
    sent, own_projection, own_rows = lax.optimization_barrier(
        (sent, temporal_mix_projection_matrix, whole_rows)
    )
    got = lax.all_to_all(sent, SEQ, split_axis=0, concat_axis=0, tiled=True)
    projection = [own_projection]
    for k in range(1, 4):
        projection.append(lax.ppermute(own_projection, MP, [(i, i ^ k) for i in range(4)]))
    other_rows = lax.ppermute(own_rows, "x_lo", [(0, 1), (1, 0)])
    first_half = lax.axis_index("x_lo") == 0
    both_rows = jnp.stack(
        [jnp.where(first_half, own_rows, other_rows), jnp.where(first_half, other_rows, own_rows)]
    )
    height = got.shape[0]
    got = got.reshape(height, 4, inner_width)
    col_out = recurrence(
        got[None, :, 0],
        got[None, :, 1],
        got[None, :, 2],
        got[None, :, 3],
        self_token_reward,
        vertical_cluster_scaling,
    )[0]
    col_sent = col_out.reshape(height, inner_width // 128, 128)
    col_sent, projection, both_rows = lax.optimization_barrier((col_sent, projection, both_rows))
    back = lax.all_to_all(col_sent, SEQ, split_axis=0, concat_axis=0, tiled=True)
    back = back.reshape(full_cols, inner_width)
    groups = from_everyone(back, MIX).reshape(2, 4, full_cols, inner_width)
    group = lax.axis_index(MP)
    attended = jnp.zeros((2 * full_cols, model_width), jnp.float32)
    for k in range(4):
        one = lax.dynamic_index_in_dim(groups, group ^ k, 1, keepdims=False)
        attended = attended + jnp.dot(
            one.reshape(2 * full_cols, inner_width),
            projection[k],
            preferred_element_type=jnp.float32,
        )
    both_rows = both_rows.reshape(2 * full_cols, model_width)
    residual_all = (both_rows.astype(jnp.float32) + attended).astype(jnp.bfloat16)
    residual = lax.dynamic_slice_in_dim(
        residual_all, lax.axis_index(MIX) * part_cols, part_cols, 0
    )
    mix_all = layer_norm(residual_all, later_standardize_scaling)

    places = unit_order(planes, depth, width)
    moved = (jnp.arange(model_width)[:, None] == places[None, :]).astype(jnp.bfloat16)
    mix_all = jnp.dot(mix_all, moved, preferred_element_type=jnp.float32).astype(jnp.bfloat16)
    hidden_pre = jnp.dot(mix_all, weights, preferred_element_type=jnp.float32)
    positive = jnp.maximum(hidden_pre[:, : units // 2], 0.0)
    hidden = (positive * positive).astype(jnp.bfloat16)
    hidden = jnp.pad(hidden, ((0, 0), (units // 2, 0)))
    downward = lax.dot_general(
        hidden, weights, (((1,), (1,)), ((), ())), preferred_element_type=jnp.float32
    ).astype(jnp.bfloat16)
    downward = lax.dot_general(
        downward, moved, (((1,), (1,)), ((), ())), preferred_element_type=jnp.float32
    ).astype(jnp.bfloat16)
    mixed = sent_and_summed(downward, MIX, 0)
    block_out = (residual.astype(jnp.float32) + mixed).astype(jnp.bfloat16)
    return block_out.reshape(images, row_count, part_cols, model_width)


def solution(mesh):
    torus = Mesh(mesh.devices.reshape(2, 4, 16, 2, 2), (*SEQ, *MP))
    return jax.shard_map(
        shards,
        mesh=torus,
        in_specs=(
            P(None, SEQ, MP, None),
            P(),
            P(None, MP),
            P(None, MP),
            P(None, MP),
            P(),
            P(None, MP),
            P(MP),
            P(MP),
            P(MP),
            P(MP),
            P(MP, None),
            P(),
            P(SEQ, MP),
            P(MP, SEQ),
        ),
        out_specs=P(None, SEQ, MP, None),
        check_vma=False,
    )
```

```python
import jax
import jax.numpy as jnp
from jax import lax
from jax.sharding import Mesh
from jax.sharding import PartitionSpec as P


SUBSPACE_SIZE = 64
SEQ = ("x_lo", "y", "z")
MP = ("x_hi", "core")
PLANE = ("x_lo", "y")


def from_everyone(value, axis):
    copies = jnp.broadcast_to(value, (lax.axis_size(axis), *value.shape))
    return lax.all_to_all(copies, axis, split_axis=0, concat_axis=0, tiled=True)


def split_up(value, dim, size):
    lengths = value.shape
    pieces = value.reshape(*lengths[:dim], size, lengths[dim] // size, *lengths[dim + 1 :])
    return jnp.moveaxis(pieces, dim, 0)


def sent_and_summed(value, axis, dim):
    size = lax.axis_size(axis)
    pieces = lax.all_to_all(split_up(value, dim, size), axis, 0, 0, tiled=True)
    return jnp.sum(pieces.astype(jnp.float32), axis=0)


def layer_norm(inputs, gain):
    values = inputs.astype(jnp.float32)
    average = jnp.mean(values, axis=-1, keepdims=True)
    centred = values - average
    spread = jnp.mean(centred * centred, axis=-1, keepdims=True)
    return (centred * lax.rsqrt(spread + 1e-05) * gain).astype(jnp.bfloat16)


def heads_first(array, nheads):
    number, length, inner_width = array.shape
    shaped = array.astype(jnp.float32).reshape(number, length, nheads, inner_width // nheads)
    return shaped.transpose(0, 2, 1, 3)


def recurrence(recept_in, keying_in, decays_in, valued_in, boost_in, gain):
    number, length, inner_width = recept_in.shape
    nheads = inner_width // SUBSPACE_SIZE
    head_size = inner_width // nheads
    blocks = length // 16
    acceptance_horizontal_lines = heads_first(recept_in, nheads)
    addressing_horizontal_lines = heads_first(keying_in, nheads)
    decays = heads_first(decays_in, nheads)
    content_horizontal_lines = heads_first(valued_in, nheads)
    boost = boost_in.reshape(nheads, 1, head_size)
    running = jnp.cumsum(decays, axis=2)
    before = running - decays
    before_blocks = before.reshape(number, nheads, blocks, 16, head_size)
    anchor = before_blocks[:, :, :, :1, :]
    queries = acceptance_horizontal_lines.reshape(number, nheads, blocks, 16, head_size) * jnp.exp(
        before_blocks - anchor
    )
    places = jnp.arange(length)
    limits = (jnp.arange(blocks) + 1) * 16
    usable = places[None, :] < limits[:, None]
    exponent = anchor - running[:, :, None, :, :]
    exponent = jnp.where(usable[None, None, :, :, None], exponent, -10000.0)
    weighted = addressing_horizontal_lines[:, :, None, :, :] * jnp.exp(exponent)
    scores = jnp.einsum("nhbqc,nhbsc->nhbqs", queries, weighted, precision=lax.Precision.HIGHEST)
    query_places = places.reshape(blocks, 16)
    earlier = places[None, None, :] < query_places[:, :, None]
    scores = jnp.where(earlier[None, None], scores, 0.0)
    current = jnp.sum(acceptance_horizontal_lines * boost * addressing_horizontal_lines, axis=-1)
    summed = jnp.einsum(
        "nhbqs,nhsc->nhbqc", scores, content_horizontal_lines, precision=lax.Precision.HIGHEST
    )
    summed = (
        summed.reshape(number, nheads, length, head_size)
        + current[..., None] * content_horizontal_lines
    )
    average = jnp.mean(summed, axis=-1, keepdims=True)
    centred = summed - average
    spread = jnp.mean(centred * centred, axis=-1, keepdims=True)
    normed = (
        (centred * lax.rsqrt(spread + 0.00064))
        .transpose(0, 2, 1, 3)
        .reshape(number, length, inner_width)
    )
    return (normed * gain).astype(jnp.bfloat16)


def unit_order(planes, depth, width):
    stored = jnp.arange(planes * depth * width)
    z, rest = stored // (planes * width), stored % (planes * width)
    plane, row = rest // width, rest % width
    true_place = (plane * depth + z) * width + row
    return true_place


def shards(
    incoming_image_patches,
    initial_standardize_scaling,
    acceptance_matrix,
    addressing_matrix,
    content_matrix,
    forgetting_lowdim_left_factor,
    forgetting_lowdim_right_factor,
    forgetting_baseline,
    self_token_reward,
    horizontal_cluster_scaling,
    vertical_cluster_scaling,
    temporal_mix_projection_matrix,
    later_standardize_scaling,
    feature_mix_addressing_matrix,
    feature_mix_content_matrix,
):
    images, row_count, part_cols, model_width = incoming_image_patches.shape
    tokens = incoming_image_patches.reshape(part_cols, model_width)
    whole_rows = lax.all_gather(tokens, MP, axis=0, tiled=True)
    full_cols = whole_rows.shape[0]
    inner_width = acceptance_matrix.shape[1]

    planes, depth = lax.axis_size(PLANE), lax.axis_size("z")
    width = feature_mix_addressing_matrix.shape[0]
    pair = jnp.stack([feature_mix_addressing_matrix, feature_mix_content_matrix.T])
    plane_pair = from_everyone(pair, PLANE)
    plane_pair = plane_pair.reshape(planes, *pair.shape)
    plane_pair = jnp.swapaxes(plane_pair, 0, 1).reshape(2 * planes * width, -1)
    full_pair = lax.all_gather(plane_pair, "z", axis=0, tiled=True)
    full_pair = full_pair.reshape(depth, 2, planes * width, -1)
    full_up = full_pair[:, 0].reshape(model_width, -1)
    full_down = full_pair[:, 1].reshape(model_width, -1)

    xn1 = layer_norm(whole_rows, initial_standardize_scaling)
    recept = jnp.dot(xn1, acceptance_matrix, preferred_element_type=jnp.float32).astype(
        jnp.bfloat16
    )
    keying = jnp.dot(xn1, addressing_matrix, preferred_element_type=jnp.float32).astype(
        jnp.bfloat16
    )
    valued = jnp.dot(xn1, content_matrix, preferred_element_type=jnp.float32).astype(jnp.bfloat16)
    latent = jnp.tanh(
        jnp.dot(xn1, forgetting_lowdim_left_factor, preferred_element_type=jnp.float32)
    ).astype(jnp.bfloat16)
    decay = (
        -0.7
        * jax.nn.sigmoid(
            forgetting_baseline
            + jnp.dot(latent, forgetting_lowdim_right_factor, preferred_element_type=jnp.float32)
        )
    ).astype(jnp.bfloat16)
    row_out = recurrence(
        recept[None],
        keying[None],
        decay[None],
        valued[None],
        self_token_reward,
        horizontal_cluster_scaling,
    )[0]
    sent = jnp.stack([recept, keying, decay, row_out], axis=1)
    sent = sent.reshape(full_cols, 4 * inner_width // 128, 128)
    got = lax.all_to_all(sent, SEQ, split_axis=0, concat_axis=0, tiled=True)
    height = got.shape[0]
    got = got.reshape(height, 4, inner_width)
    col_out = recurrence(
        got[None, :, 0],
        got[None, :, 1],
        got[None, :, 2],
        got[None, :, 3],
        self_token_reward,
        vertical_cluster_scaling,
    )[0]
    back = lax.all_to_all(
        col_out.reshape(height, inner_width // 128, 128),
        SEQ,
        split_axis=0,
        concat_axis=0,
        tiled=True,
    ).reshape(full_cols, inner_width)
    partial_value = jnp.dot(
        back, temporal_mix_projection_matrix, preferred_element_type=jnp.float32
    ).astype(jnp.bfloat16)
    attended = sent_and_summed(partial_value, MP, 0)
    residual = (tokens.astype(jnp.float32) + attended).astype(jnp.bfloat16)
    mix_input = layer_norm(residual, later_standardize_scaling)

    places = unit_order(planes, depth, width)
    moved = (jnp.arange(model_width)[:, None] == places[None, :]).astype(jnp.bfloat16)
    mix_input = jnp.dot(mix_input, moved, preferred_element_type=jnp.float32).astype(jnp.bfloat16)
    mix_all = lax.all_gather(mix_input, MP, axis=0, tiled=True)
    hidden_pre = jnp.dot(mix_all, full_up, preferred_element_type=jnp.float32)
    positive = jnp.maximum(hidden_pre, 0.0)
    hidden = (positive * positive).astype(jnp.bfloat16)
    downward = lax.dot_general(
        hidden, full_down, (((1,), (1,)), ((), ())), preferred_element_type=jnp.float32
    ).astype(jnp.bfloat16)
    downward = lax.dot_general(
        downward, moved, (((1,), (1,)), ((), ())), preferred_element_type=jnp.float32
    ).astype(jnp.bfloat16)
    mixed = sent_and_summed(downward, MP, 0)
    block_out = (residual.astype(jnp.float32) + mixed).astype(jnp.bfloat16)
    return block_out.reshape(images, row_count, part_cols, model_width)


def solution(mesh):
    torus = Mesh(mesh.devices.reshape(2, 4, 16, 2, 2), (*SEQ, *MP))
    return jax.shard_map(
        shards,
        mesh=torus,
        in_specs=(
            P(None, SEQ, MP, None),
            P(),
            P(None, MP),
            P(None, MP),
            P(None, MP),
            P(),
            P(None, MP),
            P(MP),
            P(MP),
            P(MP),
            P(MP),
            P(MP, None),
            P(),
            P(SEQ, MP),
            P(MP, SEQ),
        ),
        out_specs=P(None, SEQ, MP, None),
        check_vma=False,
    )
```

```python
import jax
import jax.numpy as jnp
from jax import lax
from jax.sharding import Mesh
from jax.sharding import PartitionSpec as P


SUBSPACE_SIZE = 64
SEQ = ("x_lo", "y", "z")
MP = ("x_hi", "core")
PLANE = ("x_lo", "y")
MIX = ("x_lo", "x_hi", "core")


def from_everyone(value, axis):
    copies = jnp.broadcast_to(value, (lax.axis_size(axis), *value.shape))
    return lax.all_to_all(copies, axis, split_axis=0, concat_axis=0, tiled=True)


def split_up(value, dim, size):
    lengths = value.shape
    pieces = value.reshape(*lengths[:dim], size, lengths[dim] // size, *lengths[dim + 1 :])
    return jnp.moveaxis(pieces, dim, 0)


def sent_and_summed(value, axis, dim):
    size = lax.axis_size(axis)
    pieces = lax.all_to_all(split_up(value, dim, size), axis, 0, 0, tiled=True)
    return jnp.sum(pieces.astype(jnp.float32), axis=0)


def layer_norm(inputs, gain):
    values = inputs.astype(jnp.float32)
    average = jnp.mean(values, axis=-1, keepdims=True)
    centred = values - average
    spread = jnp.mean(centred * centred, axis=-1, keepdims=True)
    return (centred * lax.rsqrt(spread + 1e-05) * gain).astype(jnp.bfloat16)


def heads_first(array, nheads):
    number, length, inner_width = array.shape
    shaped = array.astype(jnp.float32).reshape(number, length, nheads, inner_width // nheads)
    return shaped.transpose(0, 2, 1, 3)


def recurrence(recept_in, keying_in, decays_in, valued_in, boost_in, gain):
    number, length, inner_width = recept_in.shape
    nheads = inner_width // SUBSPACE_SIZE
    head_size = inner_width // nheads
    blocks = length // 16
    acceptance_horizontal_lines = heads_first(recept_in, nheads)
    addressing_horizontal_lines = heads_first(keying_in, nheads)
    decays = heads_first(decays_in, nheads)
    content_horizontal_lines = heads_first(valued_in, nheads)
    boost = boost_in.reshape(nheads, 1, head_size)
    running = jnp.cumsum(decays, axis=2)
    before = running - decays
    before_blocks = before.reshape(number, nheads, blocks, 16, head_size)
    anchor = before_blocks[:, :, :, :1, :]
    queries = acceptance_horizontal_lines.reshape(number, nheads, blocks, 16, head_size) * jnp.exp(
        before_blocks - anchor
    )
    places = jnp.arange(length)
    limits = (jnp.arange(blocks) + 1) * 16
    usable = places[None, :] < limits[:, None]
    exponent = anchor - running[:, :, None, :, :]
    exponent = jnp.where(usable[None, None, :, :, None], exponent, -10000.0)
    weighted = addressing_horizontal_lines[:, :, None, :, :] * jnp.exp(exponent)
    scores = jnp.einsum("nhbqc,nhbsc->nhbqs", queries, weighted, precision=lax.Precision.HIGHEST)
    query_places = places.reshape(blocks, 16)
    earlier = places[None, None, :] < query_places[:, :, None]
    scores = jnp.where(earlier[None, None], scores, 0.0)
    current = jnp.sum(acceptance_horizontal_lines * boost * addressing_horizontal_lines, axis=-1)
    summed = jnp.einsum(
        "nhbqs,nhsc->nhbqc", scores, content_horizontal_lines, precision=lax.Precision.HIGHEST
    )
    summed = (
        summed.reshape(number, nheads, length, head_size)
        + current[..., None] * content_horizontal_lines
    )
    average = jnp.mean(summed, axis=-1, keepdims=True)
    centred = summed - average
    spread = jnp.mean(centred * centred, axis=-1, keepdims=True)
    normed = (
        (centred * lax.rsqrt(spread + 0.00064))
        .transpose(0, 2, 1, 3)
        .reshape(number, length, inner_width)
    )
    return (normed * gain).astype(jnp.bfloat16)


def unit_order(planes, depth, width):
    stored = jnp.arange(planes * depth * width)
    z, rest = stored // (planes * width), stored % (planes * width)
    return ((rest // width) * depth + z) * width + rest % width


def shards(
    incoming_image_patches,
    initial_standardize_scaling,
    acceptance_matrix,
    addressing_matrix,
    content_matrix,
    forgetting_lowdim_left_factor,
    forgetting_lowdim_right_factor,
    forgetting_baseline,
    self_token_reward,
    horizontal_cluster_scaling,
    vertical_cluster_scaling,
    temporal_mix_projection_matrix,
    later_standardize_scaling,
    feature_mix_addressing_matrix,
    feature_mix_content_matrix,
):
    images, row_count, part_cols, model_width = incoming_image_patches.shape
    tokens = incoming_image_patches.reshape(part_cols, model_width)
    whole_rows = lax.all_gather(tokens, MP, axis=0, tiled=True)
    full_cols = whole_rows.shape[0]
    inner_width = acceptance_matrix.shape[1]

    planes, depth, ring = lax.axis_size(PLANE), lax.axis_size("z"), lax.axis_size("y")
    width, units = feature_mix_addressing_matrix.shape
    halves = [
        jnp.concatenate(
            [
                feature_mix_addressing_matrix[:, start : start + units // 2],
                feature_mix_content_matrix.T[:, start : start + units // 2],
            ],
            axis=1,
        )
        for start in (0, units // 2)
    ]
    halves = jnp.stack(halves)
    halves, whole_rows = lax.optimization_barrier((halves, whole_rows))
    shares = jnp.broadcast_to(halves[:, None], (2, ring, width, units))
    plane = lax.all_to_all(shares.reshape(planes, width, units), PLANE, 0, 0, tiled=True)
    plane = plane.reshape(planes * width, units)
    weights = lax.all_gather(plane, "z", axis=0, tiled=True)

    xn1 = layer_norm(whole_rows, initial_standardize_scaling)
    recept = jnp.dot(xn1, acceptance_matrix, preferred_element_type=jnp.float32).astype(
        jnp.bfloat16
    )
    keying = jnp.dot(xn1, addressing_matrix, preferred_element_type=jnp.float32).astype(
        jnp.bfloat16
    )
    valued = jnp.dot(xn1, content_matrix, preferred_element_type=jnp.float32).astype(jnp.bfloat16)
    latent = jnp.tanh(
        jnp.dot(xn1, forgetting_lowdim_left_factor, preferred_element_type=jnp.float32)
    ).astype(jnp.bfloat16)
    decay = (
        -0.7
        * jax.nn.sigmoid(
            forgetting_baseline
            + jnp.dot(latent, forgetting_lowdim_right_factor, preferred_element_type=jnp.float32)
        )
    ).astype(jnp.bfloat16)
    row_out = recurrence(
        recept[None],
        keying[None],
        decay[None],
        valued[None],
        self_token_reward,
        horizontal_cluster_scaling,
    )[0]
    sent = jnp.stack([recept, keying, decay, row_out], axis=1)
    sent = sent.reshape(full_cols, 4 * inner_width // 128, 128)
    got = lax.all_to_all(sent, SEQ, split_axis=0, concat_axis=0, tiled=True)
    height = got.shape[0]
    got = got.reshape(height, 4, inner_width)
    col_out = recurrence(
        got[None, :, 0],
        got[None, :, 1],
        got[None, :, 2],
        got[None, :, 3],
        self_token_reward,
        vertical_cluster_scaling,
    )[0]
    col_sent = col_out.reshape(height, inner_width // 128, 128)
    back = lax.all_to_all(col_sent, SEQ, split_axis=0, concat_axis=0, tiled=True)
    back = back.reshape(full_cols, inner_width)
    partial_value = jnp.dot(
        back, temporal_mix_projection_matrix, preferred_element_type=jnp.float32
    ).astype(jnp.bfloat16)
    attended = sent_and_summed(partial_value, MP, 0)
    residual = (tokens.astype(jnp.float32) + attended).astype(jnp.bfloat16)
    mix_input = layer_norm(residual, later_standardize_scaling)

    places = unit_order(planes, depth, width)
    moved = (jnp.arange(model_width)[:, None] == places[None, :]).astype(jnp.bfloat16)
    mix_input = jnp.dot(mix_input, moved, preferred_element_type=jnp.float32).astype(jnp.bfloat16)
    mix_all = from_everyone(mix_input, MIX).reshape(-1, model_width)
    hidden_pre = jnp.dot(mix_all, weights, preferred_element_type=jnp.float32)
    positive = jnp.maximum(hidden_pre[:, : units // 2], 0.0)
    hidden = (positive * positive).astype(jnp.bfloat16)
    hidden = jnp.pad(hidden, ((0, 0), (units // 2, 0)))
    downward = lax.dot_general(
        hidden, weights, (((1,), (1,)), ((), ())), preferred_element_type=jnp.float32
    ).astype(jnp.bfloat16)
    downward = lax.dot_general(
        downward, moved, (((1,), (1,)), ((), ())), preferred_element_type=jnp.float32
    ).astype(jnp.bfloat16)
    mixed = sent_and_summed(downward, MIX, 0)
    block_out = (residual.astype(jnp.float32) + mixed).astype(jnp.bfloat16)
    return block_out.reshape(images, row_count, part_cols, model_width)


def solution(mesh):
    torus = Mesh(mesh.devices.reshape(2, 4, 16, 2, 2), (*SEQ, *MP))
    return jax.shard_map(
        shards,
        mesh=torus,
        in_specs=(
            P(None, SEQ, MP, None),
            P(),
            P(None, MP),
            P(None, MP),
            P(None, MP),
            P(),
            P(None, MP),
            P(MP),
            P(MP),
            P(MP),
            P(MP),
            P(MP, None),
            P(),
            P(SEQ, MP),
            P(MP, SEQ),
        ),
        out_specs=P(None, SEQ, MP, None),
        check_vma=False,
    )
```

```python
import jax
import jax.numpy as jnp
from jax import lax
from jax.experimental import pallas as pl
from jax.sharding import Mesh
from jax.sharding import PartitionSpec as P


SUBSPACE_SIZE = 64
SEQ = ("x_lo", "y", "z")
MP = ("x_hi", "core")
PLANE = ("x_lo", "y")


def split_up(value, dim, size):
    lengths = value.shape
    pieces = value.reshape(*lengths[:dim], size, lengths[dim] // size, *lengths[dim + 1 :])
    return jnp.moveaxis(pieces, dim, 0)


def sent_and_summed(value, axis, dim):
    size = lax.axis_size(axis)
    pieces = lax.all_to_all(split_up(value, dim, size), axis, 0, 0, tiled=True)
    return jnp.sum(pieces.astype(jnp.float32), axis=0)


def layer_norm(inputs, gain):
    values = inputs.astype(jnp.float32)
    average = jnp.mean(values, axis=-1, keepdims=True)
    centred = values - average
    spread = jnp.mean(centred * centred, axis=-1, keepdims=True)
    return (centred * lax.rsqrt(spread + 1e-05) * gain).astype(jnp.bfloat16)


def heads_first(array, nheads):
    number, length, inner_width = array.shape
    shaped = array.astype(jnp.float32).reshape(number, length, nheads, inner_width // nheads)
    return shaped.transpose(0, 2, 1, 3)


def recurrence(recept_in, keying_in, decays_in, valued_in, boost_in, gain):
    number, length, inner_width = recept_in.shape
    nheads = inner_width // SUBSPACE_SIZE
    head_size = inner_width // nheads
    blocks = length // 16
    acceptance_horizontal_lines = heads_first(recept_in, nheads)
    addressing_horizontal_lines = heads_first(keying_in, nheads)
    decays = heads_first(decays_in, nheads)
    content_horizontal_lines = heads_first(valued_in, nheads)
    boost = boost_in.reshape(nheads, 1, head_size)
    running = jnp.cumsum(decays, axis=2)
    before = running - decays
    before_blocks = before.reshape(number, nheads, blocks, 16, head_size)
    anchor = before_blocks[:, :, :, :1, :]
    queries = acceptance_horizontal_lines.reshape(number, nheads, blocks, 16, head_size) * jnp.exp(
        before_blocks - anchor
    )
    places = jnp.arange(length)
    limits = (jnp.arange(blocks) + 1) * 16
    usable = places[None, :] < limits[:, None]
    exponent = anchor - running[:, :, None, :, :]
    exponent = jnp.where(usable[None, None, :, :, None], exponent, -10000.0)
    weighted = addressing_horizontal_lines[:, :, None, :, :] * jnp.exp(exponent)
    scores = jnp.einsum("nhbqc,nhbsc->nhbqs", queries, weighted, precision=lax.Precision.HIGHEST)
    query_places = places.reshape(blocks, 16)
    earlier = places[None, None, :] < query_places[:, :, None]
    scores = jnp.where(earlier[None, None], scores, 0.0)
    current = jnp.sum(acceptance_horizontal_lines * boost * addressing_horizontal_lines, axis=-1)
    summed = jnp.einsum(
        "nhbqs,nhsc->nhbqc", scores, content_horizontal_lines, precision=lax.Precision.HIGHEST
    )
    summed = (
        summed.reshape(number, nheads, length, head_size)
        + current[..., None] * content_horizontal_lines
    )
    average = jnp.mean(summed, axis=-1, keepdims=True)
    centred = summed - average
    spread = jnp.mean(centred * centred, axis=-1, keepdims=True)
    normed = (
        (centred * lax.rsqrt(spread + 0.00064))
        .transpose(0, 2, 1, 3)
        .reshape(number, length, inner_width)
    )
    return (normed * gain).astype(jnp.bfloat16)


def copies_body(up_ref, down_ref, out_ref):
    units = up_ref.shape[1]
    for plane in range(out_ref.shape[0]):
        out_ref[plane, :, :units] = up_ref[...]
        out_ref[plane, :, units:] = down_ref[...]


def side_by_side(up, down, planes):
    width, units = up.shape
    return pl.pallas_call(
        copies_body,
        out_shape=jax.ShapeDtypeStruct((planes, width, 2 * units), up.dtype),
        name="side_by_side",
    )(up, down)


def unit_order(planes, depth, width):
    stored = jnp.arange(planes * depth * width)
    z, rest = stored // (planes * width), stored % (planes * width)
    plane, row = rest // width, rest % width
    true_place = (plane * depth + z) * width + row
    return true_place


def shards(
    incoming_image_patches,
    initial_standardize_scaling,
    acceptance_matrix,
    addressing_matrix,
    content_matrix,
    forgetting_lowdim_left_factor,
    forgetting_lowdim_right_factor,
    forgetting_baseline,
    self_token_reward,
    horizontal_cluster_scaling,
    vertical_cluster_scaling,
    temporal_mix_projection_matrix,
    later_standardize_scaling,
    feature_mix_addressing_matrix,
    feature_mix_content_matrix,
):
    images, row_count, part_cols, model_width = incoming_image_patches.shape
    tokens = incoming_image_patches.reshape(part_cols, model_width)
    planes, depth = lax.axis_size(PLANE), lax.axis_size("z")
    width, units = feature_mix_addressing_matrix.shape
    copies = side_by_side(
        feature_mix_addressing_matrix, feature_mix_content_matrix.T, planes
    )
    plane_pair = lax.all_to_all(copies, PLANE, 0, 0, tiled=True)
    plane_pair = plane_pair.reshape(planes * width, 2 * units)
    plane_pair, tokens_then = lax.optimization_barrier((plane_pair, tokens))
    full_pair = lax.all_gather(plane_pair, "z", axis=0, tiled=True)

    whole_rows = lax.all_gather(tokens_then, MP, axis=0, tiled=True)
    full_cols = whole_rows.shape[0]
    inner_width = acceptance_matrix.shape[1]

    xn1 = layer_norm(whole_rows, initial_standardize_scaling)
    recept = jnp.dot(xn1, acceptance_matrix, preferred_element_type=jnp.float32).astype(
        jnp.bfloat16
    )
    keying = jnp.dot(xn1, addressing_matrix, preferred_element_type=jnp.float32).astype(
        jnp.bfloat16
    )
    valued = jnp.dot(xn1, content_matrix, preferred_element_type=jnp.float32).astype(jnp.bfloat16)
    latent = jnp.tanh(
        jnp.dot(xn1, forgetting_lowdim_left_factor, preferred_element_type=jnp.float32)
    ).astype(jnp.bfloat16)
    decay = (
        -0.7
        * jax.nn.sigmoid(
            forgetting_baseline
            + jnp.dot(latent, forgetting_lowdim_right_factor, preferred_element_type=jnp.float32)
        )
    ).astype(jnp.bfloat16)
    row_out = recurrence(
        recept[None],
        keying[None],
        decay[None],
        valued[None],
        self_token_reward,
        horizontal_cluster_scaling,
    )[0]
    sent = jnp.stack([recept, keying, decay, row_out], axis=1)
    sent = sent.reshape(full_cols, 4 * inner_width // 128, 128)
    got = lax.all_to_all(sent, SEQ, split_axis=0, concat_axis=0, tiled=True)
    height = got.shape[0]
    got = got.reshape(height, 4, inner_width)
    col_out = recurrence(
        got[None, :, 0],
        got[None, :, 1],
        got[None, :, 2],
        got[None, :, 3],
        self_token_reward,
        vertical_cluster_scaling,
    )[0]
    back = lax.all_to_all(
        col_out.reshape(height, inner_width // 128, 128),
        SEQ,
        split_axis=0,
        concat_axis=0,
        tiled=True,
    ).reshape(full_cols, inner_width)
    partial_value = jnp.dot(
        back, temporal_mix_projection_matrix, preferred_element_type=jnp.float32
    ).astype(jnp.bfloat16)
    attended = sent_and_summed(partial_value, MP, 0)
    residual = (tokens.astype(jnp.float32) + attended).astype(jnp.bfloat16)
    mix_input = layer_norm(residual, later_standardize_scaling)

    places = unit_order(planes, depth, width)
    moved = (jnp.arange(model_width)[:, None] == places[None, :]).astype(jnp.bfloat16)
    mix_input = jnp.dot(mix_input, moved, preferred_element_type=jnp.float32).astype(jnp.bfloat16)
    mix_all = lax.all_gather(mix_input, MP, axis=0, tiled=True)
    hidden_pre = jnp.dot(mix_all, full_pair[:, :units], preferred_element_type=jnp.float32)
    positive = jnp.maximum(hidden_pre, 0.0)
    hidden = (positive * positive).astype(jnp.bfloat16)
    downward = lax.dot_general(
        hidden, full_pair[:, units:], (((1,), (1,)), ((), ())), preferred_element_type=jnp.float32
    ).astype(jnp.bfloat16)
    downward = lax.dot_general(
        downward, moved, (((1,), (1,)), ((), ())), preferred_element_type=jnp.float32
    ).astype(jnp.bfloat16)
    mixed = sent_and_summed(downward, MP, 0)
    block_out = (residual.astype(jnp.float32) + mixed).astype(jnp.bfloat16)
    return block_out.reshape(images, row_count, part_cols, model_width)


def solution(mesh):
    torus = Mesh(mesh.devices.reshape(2, 4, 16, 2, 2), (*SEQ, *MP))
    return jax.shard_map(
        shards,
        mesh=torus,
        in_specs=(
            P(None, SEQ, MP, None),
            P(),
            P(None, MP),
            P(None, MP),
            P(None, MP),
            P(),
            P(None, MP),
            P(MP),
            P(MP),
            P(MP),
            P(MP),
            P(MP, None),
            P(),
            P(SEQ, MP),
            P(MP, SEQ),
        ),
        out_specs=P(None, SEQ, MP, None),
        check_vma=False,
    )
```

```python
import jax
import jax.numpy as jnp
from jax import lax
from jax.sharding import Mesh
from jax.sharding import PartitionSpec as P


SUBSPACE_SIZE = 64
SEQ = ("x_lo", "y", "z")
MP = ("x_hi", "core")
PLANE = ("x_lo", "y")


def from_everyone(value, axis):
    copies = jnp.broadcast_to(value, (lax.axis_size(axis), *value.shape))
    return lax.all_to_all(copies, axis, split_axis=0, concat_axis=0, tiled=True)


def split_up(value, dim, size):
    lengths = value.shape
    pieces = value.reshape(*lengths[:dim], size, lengths[dim] // size, *lengths[dim + 1 :])
    return jnp.moveaxis(pieces, dim, 0)


def sent_and_summed(value, axis, dim):
    size = lax.axis_size(axis)
    pieces = lax.all_to_all(split_up(value, dim, size), axis, 0, 0, tiled=True)
    return jnp.sum(pieces.astype(jnp.float32), axis=0)


def layer_norm(inputs, gain):
    values = inputs.astype(jnp.float32)
    average = jnp.mean(values, axis=-1, keepdims=True)
    centred = values - average
    spread = jnp.mean(centred * centred, axis=-1, keepdims=True)
    return (centred * lax.rsqrt(spread + 1e-05) * gain).astype(jnp.bfloat16)


def heads_first(array, nheads):
    number, length, inner_width = array.shape
    shaped = array.astype(jnp.float32).reshape(number, length, nheads, inner_width // nheads)
    return shaped.transpose(0, 2, 1, 3)


def recurrence(recept_in, keying_in, decays_in, valued_in, boost_in, gain):
    number, length, inner_width = recept_in.shape
    nheads = inner_width // SUBSPACE_SIZE
    head_size = inner_width // nheads
    blocks = length // 16
    acceptance_horizontal_lines = heads_first(recept_in, nheads)
    addressing_horizontal_lines = heads_first(keying_in, nheads)
    decays = heads_first(decays_in, nheads)
    content_horizontal_lines = heads_first(valued_in, nheads)
    boost = boost_in.reshape(nheads, 1, head_size)
    running = jnp.cumsum(decays, axis=2)
    before = running - decays
    before_blocks = before.reshape(number, nheads, blocks, 16, head_size)
    anchor = before_blocks[:, :, :, :1, :]
    queries = acceptance_horizontal_lines.reshape(number, nheads, blocks, 16, head_size) * jnp.exp(
        before_blocks - anchor
    )
    places = jnp.arange(length)
    limits = (jnp.arange(blocks) + 1) * 16
    usable = places[None, :] < limits[:, None]
    exponent = anchor - running[:, :, None, :, :]
    exponent = jnp.where(usable[None, None, :, :, None], exponent, -10000.0)
    weighted = addressing_horizontal_lines[:, :, None, :, :] * jnp.exp(exponent)
    scores = jnp.einsum("nhbqc,nhbsc->nhbqs", queries, weighted, precision=lax.Precision.HIGHEST)
    query_places = places.reshape(blocks, 16)
    earlier = places[None, None, :] < query_places[:, :, None]
    scores = jnp.where(earlier[None, None], scores, 0.0)
    current = jnp.sum(acceptance_horizontal_lines * boost * addressing_horizontal_lines, axis=-1)
    summed = jnp.einsum(
        "nhbqs,nhsc->nhbqc", scores, content_horizontal_lines, precision=lax.Precision.HIGHEST
    )
    summed = (
        summed.reshape(number, nheads, length, head_size)
        + current[..., None] * content_horizontal_lines
    )
    average = jnp.mean(summed, axis=-1, keepdims=True)
    centred = summed - average
    spread = jnp.mean(centred * centred, axis=-1, keepdims=True)
    normed = (
        (centred * lax.rsqrt(spread + 0.00064))
        .transpose(0, 2, 1, 3)
        .reshape(number, length, inner_width)
    )
    return (normed * gain).astype(jnp.bfloat16)


def log_decay(latent, right_factor, baseline):
    raised = baseline + jnp.dot(latent, right_factor, preferred_element_type=jnp.float32)
    return (-0.7 * jax.nn.sigmoid(raised)).astype(jnp.bfloat16)


def unit_order(planes, depth, width):
    stored = jnp.arange(planes * depth * width)
    z, rest = stored // (planes * width), stored % (planes * width)
    plane, row = rest // width, rest % width
    true_place = (plane * depth + z) * width + row
    return true_place


def shards(
    incoming_image_patches,
    initial_standardize_scaling,
    acceptance_matrix,
    addressing_matrix,
    content_matrix,
    forgetting_lowdim_left_factor,
    forgetting_lowdim_right_factor,
    forgetting_baseline,
    self_token_reward,
    horizontal_cluster_scaling,
    vertical_cluster_scaling,
    temporal_mix_projection_matrix,
    later_standardize_scaling,
    feature_mix_addressing_matrix,
    feature_mix_content_matrix,
):
    images, row_count, part_cols, model_width = incoming_image_patches.shape
    tokens = incoming_image_patches.reshape(part_cols, model_width)
    whole_rows = lax.all_gather(tokens, MP, axis=0, tiled=True)
    full_cols = whole_rows.shape[0]
    inner_width = acceptance_matrix.shape[1]

    planes, depth = lax.axis_size(PLANE), lax.axis_size("z")
    width = feature_mix_addressing_matrix.shape[0]
    pair = jnp.concatenate([feature_mix_addressing_matrix, feature_mix_content_matrix.T], axis=1)
    units = feature_mix_addressing_matrix.shape[1]
    plane_pair = from_everyone(pair, PLANE)
    plane_pair = plane_pair.reshape(planes * width, 2 * units)
    full_pair = lax.all_gather(plane_pair, "z", axis=0, tiled=True)

    xn1 = layer_norm(whole_rows, initial_standardize_scaling)
    recept = jnp.dot(xn1, acceptance_matrix, preferred_element_type=jnp.float32).astype(
        jnp.bfloat16
    )
    keying = jnp.dot(xn1, addressing_matrix, preferred_element_type=jnp.float32).astype(
        jnp.bfloat16
    )
    valued = jnp.dot(xn1, content_matrix, preferred_element_type=jnp.float32).astype(jnp.bfloat16)
    latent = jnp.tanh(
        jnp.dot(xn1, forgetting_lowdim_left_factor, preferred_element_type=jnp.float32)
    ).astype(jnp.bfloat16)
    decay = log_decay(latent, forgetting_lowdim_right_factor, forgetting_baseline)
    row_out = recurrence(
        recept[None],
        keying[None],
        decay[None],
        valued[None],
        self_token_reward,
        horizontal_cluster_scaling,
    )[0]
    rank = latent.shape[1]
    lines = 3 * inner_width // 128 + 1
    sent = jnp.concatenate(
        [recept, keying, row_out, jnp.pad(latent, ((0, 0), (0, 128 - rank)))], axis=1
    )
    got = lax.all_to_all(
        sent.reshape(full_cols, lines, 128), SEQ, split_axis=0, concat_axis=0, tiled=True
    )
    height = got.shape[0]
    got = got.reshape(height, 128 * lines)
    col_latent = got[:, 3 * inner_width : 3 * inner_width + rank]
    col_decay = log_decay(col_latent, forgetting_lowdim_right_factor, forgetting_baseline)
    col_out = recurrence(
        got[None, :, :inner_width],
        got[None, :, inner_width : 2 * inner_width],
        col_decay[None],
        got[None, :, 2 * inner_width : 3 * inner_width],
        self_token_reward,
        vertical_cluster_scaling,
    )[0]
    back = lax.all_to_all(
        col_out.reshape(height, inner_width // 128, 128),
        SEQ,
        split_axis=0,
        concat_axis=0,
        tiled=True,
    ).reshape(full_cols, inner_width)
    partial_value = jnp.dot(
        back, temporal_mix_projection_matrix, preferred_element_type=jnp.float32
    ).astype(jnp.bfloat16)
    attended = sent_and_summed(partial_value, MP, 0)
    residual = (tokens.astype(jnp.float32) + attended).astype(jnp.bfloat16)
    mix_input = layer_norm(residual, later_standardize_scaling)

    places = unit_order(planes, depth, width)
    moved = (jnp.arange(model_width)[:, None] == places[None, :]).astype(jnp.bfloat16)
    mix_input = jnp.dot(mix_input, moved, preferred_element_type=jnp.float32).astype(jnp.bfloat16)
    mix_all = lax.all_gather(mix_input, MP, axis=0, tiled=True)
    hidden_pre = jnp.dot(mix_all, full_pair[:, :units], preferred_element_type=jnp.float32)
    positive = jnp.maximum(hidden_pre, 0.0)
    hidden = (positive * positive).astype(jnp.bfloat16)
    downward = lax.dot_general(
        hidden, full_pair[:, units:], (((1,), (1,)), ((), ())), preferred_element_type=jnp.float32
    ).astype(jnp.bfloat16)
    downward = lax.dot_general(
        downward, moved, (((1,), (1,)), ((), ())), preferred_element_type=jnp.float32
    ).astype(jnp.bfloat16)
    mixed = sent_and_summed(downward, MP, 0)
    block_out = (residual.astype(jnp.float32) + mixed).astype(jnp.bfloat16)
    return block_out.reshape(images, row_count, part_cols, model_width)


def solution(mesh):
    torus = Mesh(mesh.devices.reshape(2, 4, 16, 2, 2), (*SEQ, *MP))
    return jax.shard_map(
        shards,
        mesh=torus,
        in_specs=(
            P(None, SEQ, MP, None),
            P(),
            P(None, MP),
            P(None, MP),
            P(None, MP),
            P(),
            P(None, MP),
            P(MP),
            P(MP),
            P(MP),
            P(MP),
            P(MP, None),
            P(),
            P(SEQ, MP),
            P(MP, SEQ),
        ),
        out_specs=P(None, SEQ, MP, None),
        check_vma=False,
    )
```

```python
import jax
import jax.numpy as jnp
from jax import lax
from jax.sharding import Mesh
from jax.sharding import PartitionSpec as P


SUBSPACE_SIZE = 64
SEQ = ("x_lo", "y", "z")
MP = ("x_hi", "core")
PLANE = ("x_lo", "y")


def from_everyone(value, axis):
    copies = jnp.broadcast_to(value, (lax.axis_size(axis), *value.shape))
    return lax.all_to_all(copies, axis, split_axis=0, concat_axis=0, tiled=True)


def split_up(value, dim, size):
    lengths = value.shape
    pieces = value.reshape(*lengths[:dim], size, lengths[dim] // size, *lengths[dim + 1 :])
    return jnp.moveaxis(pieces, dim, 0)


def sent_and_summed(value, axis, dim):
    size = lax.axis_size(axis)
    pieces = lax.all_to_all(split_up(value, dim, size), axis, 0, 0, tiled=True)
    return jnp.sum(pieces.astype(jnp.float32), axis=0)


def layer_norm(inputs, gain):
    values = inputs.astype(jnp.float32)
    average = jnp.mean(values, axis=-1, keepdims=True)
    centred = values - average
    spread = jnp.mean(centred * centred, axis=-1, keepdims=True)
    return (centred * lax.rsqrt(spread + 1e-05) * gain).astype(jnp.bfloat16)


def heads_first(array, nheads):
    number, length, inner_width = array.shape
    shaped = array.astype(jnp.float32).reshape(number, length, nheads, inner_width // nheads)
    return shaped.transpose(0, 2, 1, 3)


def recurrence(recept_in, keying_in, decays_in, valued_in, boost_in, gain):
    number, length, inner_width = recept_in.shape
    nheads = inner_width // SUBSPACE_SIZE
    head_size = inner_width // nheads
    blocks = length // 16
    acceptance_horizontal_lines = heads_first(recept_in, nheads)
    addressing_horizontal_lines = heads_first(keying_in, nheads)
    decays = heads_first(decays_in, nheads)
    content_horizontal_lines = heads_first(valued_in, nheads)
    boost = boost_in.reshape(nheads, 1, head_size)
    running = jnp.cumsum(decays, axis=2)
    before = running - decays
    before_blocks = before.reshape(number, nheads, blocks, 16, head_size)
    anchor = before_blocks[:, :, :, :1, :]
    queries = acceptance_horizontal_lines.reshape(number, nheads, blocks, 16, head_size) * jnp.exp(
        before_blocks - anchor
    )
    places = jnp.arange(length)
    limits = (jnp.arange(blocks) + 1) * 16
    usable = places[None, :] < limits[:, None]
    exponent = anchor - running[:, :, None, :, :]
    exponent = jnp.where(usable[None, None, :, :, None], exponent, -10000.0)
    weighted = addressing_horizontal_lines[:, :, None, :, :] * jnp.exp(exponent)
    scores = jnp.einsum("nhbqc,nhbsc->nhbqs", queries, weighted, precision=lax.Precision.HIGHEST)
    query_places = places.reshape(blocks, 16)
    earlier = places[None, None, :] < query_places[:, :, None]
    scores = jnp.where(earlier[None, None], scores, 0.0)
    current = jnp.sum(acceptance_horizontal_lines * boost * addressing_horizontal_lines, axis=-1)
    summed = jnp.einsum(
        "nhbqs,nhsc->nhbqc", scores, content_horizontal_lines, precision=lax.Precision.HIGHEST
    )
    summed = (
        summed.reshape(number, nheads, length, head_size)
        + current[..., None] * content_horizontal_lines
    )
    average = jnp.mean(summed, axis=-1, keepdims=True)
    centred = summed - average
    spread = jnp.mean(centred * centred, axis=-1, keepdims=True)
    normed = (
        (centred * lax.rsqrt(spread + 0.00064))
        .transpose(0, 2, 1, 3)
        .reshape(number, length, inner_width)
    )
    return (normed * gain).astype(jnp.bfloat16)


def log_decay(latent, right_factor, baseline):
    raised = baseline + jnp.dot(latent, right_factor, preferred_element_type=jnp.float32)
    return (-0.7 * jax.nn.sigmoid(raised)).astype(jnp.bfloat16)


def unit_order(planes, depth, width):
    stored = jnp.arange(planes * depth * width)
    z, rest = stored // (planes * width), stored % (planes * width)
    plane, row = rest // width, rest % width
    true_place = (plane * depth + z) * width + row
    return true_place


def shards(
    incoming_image_patches,
    initial_standardize_scaling,
    acceptance_matrix,
    addressing_matrix,
    content_matrix,
    forgetting_lowdim_left_factor,
    forgetting_lowdim_right_factor,
    forgetting_baseline,
    self_token_reward,
    horizontal_cluster_scaling,
    vertical_cluster_scaling,
    temporal_mix_projection_matrix,
    later_standardize_scaling,
    feature_mix_addressing_matrix,
    feature_mix_content_matrix,
):
    images, row_count, part_cols, model_width = incoming_image_patches.shape
    tokens = incoming_image_patches.reshape(part_cols, model_width)
    whole_rows = lax.all_gather(tokens, MP, axis=0, tiled=True)
    full_cols = whole_rows.shape[0]
    inner_width = acceptance_matrix.shape[1]

    planes, depth = lax.axis_size(PLANE), lax.axis_size("z")
    width = feature_mix_addressing_matrix.shape[0]
    pair = jnp.concatenate([feature_mix_addressing_matrix, feature_mix_content_matrix.T], axis=1)
    units = feature_mix_addressing_matrix.shape[1]
    plane_pair = from_everyone(pair, PLANE)
    plane_pair = plane_pair.reshape(planes * width, 2 * units)
    full_pair = lax.all_gather(plane_pair, "z", axis=0, tiled=True)

    xn1 = layer_norm(whole_rows, initial_standardize_scaling)
    recept = jnp.dot(xn1, acceptance_matrix, preferred_element_type=jnp.float32).astype(
        jnp.bfloat16
    )
    keying = jnp.dot(xn1, addressing_matrix, preferred_element_type=jnp.float32).astype(
        jnp.bfloat16
    )
    valued = jnp.dot(xn1, content_matrix, preferred_element_type=jnp.float32).astype(jnp.bfloat16)
    latent = jnp.tanh(
        jnp.dot(xn1, forgetting_lowdim_left_factor, preferred_element_type=jnp.float32)
    ).astype(jnp.bfloat16)
    decay = log_decay(latent, forgetting_lowdim_right_factor, forgetting_baseline)
    row_out = recurrence(
        recept[None],
        keying[None],
        decay[None],
        valued[None],
        self_token_reward,
        horizontal_cluster_scaling,
    )[0]
    rank = latent.shape[1]
    lines = 3 * inner_width // 128 + 1
    sent = jnp.concatenate(
        [recept, keying, row_out, jnp.pad(latent, ((0, 0), (0, 128 - rank)))], axis=1
    )
    got = lax.all_to_all(
        sent.reshape(full_cols, lines, 128), SEQ, split_axis=0, concat_axis=0, tiled=True
    )
    height = got.shape[0]
    got = got.reshape(height, 128 * lines)
    col_latent = got[:, 3 * inner_width : 3 * inner_width + rank]
    col_decay = log_decay(col_latent, forgetting_lowdim_right_factor, forgetting_baseline)
    col_out = recurrence(
        got[None, :, :inner_width],
        got[None, :, inner_width : 2 * inner_width],
        col_decay[None],
        got[None, :, 2 * inner_width : 3 * inner_width],
        self_token_reward,
        vertical_cluster_scaling,
    )[0]
    back = lax.all_to_all(
        col_out.reshape(height, inner_width // 128, 128),
        SEQ,
        split_axis=0,
        concat_axis=0,
        tiled=True,
    ).reshape(full_cols, inner_width)
    partial_value = jnp.dot(
        back, temporal_mix_projection_matrix, preferred_element_type=jnp.float32
    ).astype(jnp.bfloat16)
    attended = sent_and_summed(partial_value, MP, 0)
    residual = (tokens.astype(jnp.float32) + attended).astype(jnp.bfloat16)
    mix_input = layer_norm(residual, later_standardize_scaling)

    places = unit_order(planes, depth, width)
    moved = (jnp.arange(model_width)[:, None] == places[None, :]).astype(jnp.bfloat16)
    mix_input = jnp.dot(mix_input, moved, preferred_element_type=jnp.float32).astype(jnp.bfloat16)
    stored_residual = jnp.dot(residual, moved, preferred_element_type=jnp.float32).astype(
        jnp.bfloat16
    )
    mix_input, stored_residual = lax.optimization_barrier((mix_input, stored_residual))
    mix_all = lax.all_gather(mix_input, MP, axis=0, tiled=True)
    hidden_pre = jnp.dot(mix_all, full_pair[:, :units], preferred_element_type=jnp.float32)
    positive = jnp.maximum(hidden_pre, 0.0)
    hidden = (positive * positive).astype(jnp.bfloat16)
    downward = lax.dot_general(
        hidden, full_pair[:, units:], (((1,), (1,)), ((), ())), preferred_element_type=jnp.float32
    ).astype(jnp.bfloat16)
    mixed = sent_and_summed(downward, MP, 0)
    stored_out = (stored_residual.astype(jnp.float32) + mixed).astype(jnp.bfloat16)
    block_out = lax.dot_general(
        stored_out, moved, (((1,), (1,)), ((), ())), preferred_element_type=jnp.float32
    ).astype(jnp.bfloat16)
    return block_out.reshape(images, row_count, part_cols, model_width)


def solution(mesh):
    torus = Mesh(mesh.devices.reshape(2, 4, 16, 2, 2), (*SEQ, *MP))
    return jax.shard_map(
        shards,
        mesh=torus,
        in_specs=(
            P(None, SEQ, MP, None),
            P(),
            P(None, MP),
            P(None, MP),
            P(None, MP),
            P(),
            P(None, MP),
            P(MP),
            P(MP),
            P(MP),
            P(MP),
            P(MP, None),
            P(),
            P(SEQ, MP),
            P(MP, SEQ),
        ),
        out_specs=P(None, SEQ, MP, None),
        check_vma=False,
    )
```

```python
import jax
import jax.numpy as jnp
from jax import lax
from jax.sharding import Mesh
from jax.sharding import PartitionSpec as P


SUBSPACE_SIZE = 64
SEQ = ("x_lo", "y", "z")
MP = ("x_hi", "core")
PLANE = ("x_lo", "y")


def from_everyone(value, axis):
    copies = jnp.broadcast_to(value, (lax.axis_size(axis), *value.shape))
    return lax.all_to_all(copies, axis, split_axis=0, concat_axis=0, tiled=True)


def split_up(value, dim, size):
    lengths = value.shape
    pieces = value.reshape(*lengths[:dim], size, lengths[dim] // size, *lengths[dim + 1 :])
    return jnp.moveaxis(pieces, dim, 0)


def sent_and_summed(value, axis, dim):
    size = lax.axis_size(axis)
    pieces = lax.all_to_all(split_up(value, dim, size), axis, 0, 0, tiled=True)
    return jnp.sum(pieces.astype(jnp.float32), axis=0)


def layer_norm(inputs, gain):
    values = inputs.astype(jnp.float32)
    average = jnp.mean(values, axis=-1, keepdims=True)
    centred = values - average
    spread = jnp.mean(centred * centred, axis=-1, keepdims=True)
    return (centred * lax.rsqrt(spread + 1e-05) * gain).astype(jnp.bfloat16)


def heads_first(array, nheads):
    number, length, inner_width = array.shape
    shaped = array.astype(jnp.float32).reshape(number, length, nheads, inner_width // nheads)
    return shaped.transpose(0, 2, 1, 3)


def recurrence(recept_in, keying_in, decays_in, valued_in, boost_in, gain):
    number, length, inner_width = recept_in.shape
    nheads = inner_width // SUBSPACE_SIZE
    head_size = inner_width // nheads
    blocks = length // 16
    acceptance_horizontal_lines = heads_first(recept_in, nheads)
    addressing_horizontal_lines = heads_first(keying_in, nheads)
    decays = heads_first(decays_in, nheads)
    content_horizontal_lines = heads_first(valued_in, nheads)
    boost = boost_in.reshape(nheads, 1, head_size)
    running = jnp.cumsum(decays, axis=2)
    before = running - decays
    before_blocks = before.reshape(number, nheads, blocks, 16, head_size)
    anchor = before_blocks[:, :, :, :1, :]
    queries = acceptance_horizontal_lines.reshape(number, nheads, blocks, 16, head_size) * jnp.exp(
        before_blocks - anchor
    )
    places = jnp.arange(length)
    limits = (jnp.arange(blocks) + 1) * 16
    usable = places[None, :] < limits[:, None]
    exponent = anchor - running[:, :, None, :, :]
    exponent = jnp.where(usable[None, None, :, :, None], exponent, -10000.0)
    weighted = addressing_horizontal_lines[:, :, None, :, :] * jnp.exp(exponent)
    scores = jnp.einsum("nhbqc,nhbsc->nhbqs", queries, weighted, precision=lax.Precision.HIGHEST)
    query_places = places.reshape(blocks, 16)
    earlier = places[None, None, :] < query_places[:, :, None]
    scores = jnp.where(earlier[None, None], scores, 0.0)
    current = jnp.sum(acceptance_horizontal_lines * boost * addressing_horizontal_lines, axis=-1)
    summed = jnp.einsum(
        "nhbqs,nhsc->nhbqc", scores, content_horizontal_lines, precision=lax.Precision.HIGHEST
    )
    summed = (
        summed.reshape(number, nheads, length, head_size)
        + current[..., None] * content_horizontal_lines
    )
    average = jnp.mean(summed, axis=-1, keepdims=True)
    centred = summed - average
    spread = jnp.mean(centred * centred, axis=-1, keepdims=True)
    normed = (
        (centred * lax.rsqrt(spread + 0.00064))
        .transpose(0, 2, 1, 3)
        .reshape(number, length, inner_width)
    )
    return (normed * gain).astype(jnp.bfloat16)


def unit_order(planes, depth, width):
    stored = jnp.arange(planes * depth * width)
    z, rest = stored // (planes * width), stored % (planes * width)
    plane, row = rest // width, rest % width
    true_place = (plane * depth + z) * width + row
    return true_place


def shards(
    incoming_image_patches,
    initial_standardize_scaling,
    acceptance_matrix,
    addressing_matrix,
    content_matrix,
    forgetting_lowdim_left_factor,
    forgetting_lowdim_right_factor,
    forgetting_baseline,
    self_token_reward,
    horizontal_cluster_scaling,
    vertical_cluster_scaling,
    temporal_mix_projection_matrix,
    later_standardize_scaling,
    feature_mix_addressing_matrix,
    feature_mix_content_matrix,
):
    images, row_count, part_cols, model_width = incoming_image_patches.shape
    tokens = incoming_image_patches.reshape(part_cols, model_width)
    whole_rows = lax.all_gather(tokens, MP, axis=0, tiled=True)
    full_cols = whole_rows.shape[0]
    inner_width = acceptance_matrix.shape[1]

    planes, depth = lax.axis_size(PLANE), lax.axis_size("z")
    width = feature_mix_addressing_matrix.shape[0]
    pair = jnp.concatenate([feature_mix_addressing_matrix, feature_mix_content_matrix.T], axis=1)
    units = feature_mix_addressing_matrix.shape[1]
    plane_pair = from_everyone(pair, PLANE)
    plane_pair = plane_pair.reshape(planes * width, 2 * units)
    full_pair = lax.all_gather(plane_pair, "z", axis=0, tiled=True)

    xn1 = layer_norm(whole_rows, initial_standardize_scaling)
    recept = jnp.dot(xn1, acceptance_matrix, preferred_element_type=jnp.float32).astype(
        jnp.bfloat16
    )
    keying = jnp.dot(xn1, addressing_matrix, preferred_element_type=jnp.float32).astype(
        jnp.bfloat16
    )
    valued = jnp.dot(xn1, content_matrix, preferred_element_type=jnp.float32).astype(jnp.bfloat16)
    latent = jnp.tanh(
        jnp.dot(xn1, forgetting_lowdim_left_factor, preferred_element_type=jnp.float32)
    ).astype(jnp.bfloat16)
    decay = (
        -0.7
        * jax.nn.sigmoid(
            forgetting_baseline
            + jnp.dot(latent, forgetting_lowdim_right_factor, preferred_element_type=jnp.float32)
        )
    ).astype(jnp.bfloat16)
    row_out = recurrence(
        recept[None],
        keying[None],
        decay[None],
        valued[None],
        self_token_reward,
        horizontal_cluster_scaling,
    )[0]
    sent = jnp.concatenate([recept, keying, decay, row_out], axis=1)
    sent = sent.reshape(full_cols, 4 * inner_width // 128, 128)
    got = lax.all_to_all(sent, SEQ, split_axis=0, concat_axis=0, tiled=True)
    height = got.shape[0]
    got = got.reshape(height, 4, inner_width)
    col_out = recurrence(
        got[None, :, 0],
        got[None, :, 1],
        got[None, :, 2],
        got[None, :, 3],
        self_token_reward,
        vertical_cluster_scaling,
    )[0]
    back = lax.all_to_all(
        col_out.reshape(height, inner_width // 128, 128),
        SEQ,
        split_axis=0,
        concat_axis=0,
        tiled=True,
    ).reshape(full_cols, inner_width)
    partial_value = jnp.dot(
        back, temporal_mix_projection_matrix, preferred_element_type=jnp.float32
    ).astype(jnp.bfloat16)
    attended = sent_and_summed(partial_value, MP, 0)
    residual = (tokens.astype(jnp.float32) + attended).astype(jnp.bfloat16)
    mix_input = layer_norm(residual, later_standardize_scaling)

    places = unit_order(planes, depth, width)
    moved = (jnp.arange(model_width)[:, None] == places[None, :]).astype(jnp.bfloat16)
    mix_input = jnp.dot(mix_input, moved, preferred_element_type=jnp.float32).astype(jnp.bfloat16)
    mix_all = lax.all_gather(mix_input, MP, axis=0, tiled=True)
    hidden_pre = jnp.dot(mix_all, full_pair[:, :units], preferred_element_type=jnp.float32)
    positive = jnp.maximum(hidden_pre, 0.0)
    hidden = (positive * positive).astype(jnp.bfloat16)
    downward = lax.dot_general(
        hidden, full_pair[:, units:], (((1,), (1,)), ((), ())), preferred_element_type=jnp.float32
    ).astype(jnp.bfloat16)
    downward = lax.dot_general(
        downward, moved, (((1,), (1,)), ((), ())), preferred_element_type=jnp.float32
    ).astype(jnp.bfloat16)
    mixed = sent_and_summed(downward, MP, 0)
    block_out = (residual.astype(jnp.float32) + mixed).astype(jnp.bfloat16)
    return block_out.reshape(images, row_count, part_cols, model_width)


def solution(mesh):
    torus = Mesh(mesh.devices.reshape(2, 4, 16, 2, 2), (*SEQ, *MP))
    return jax.shard_map(
        shards,
        mesh=torus,
        in_specs=(
            P(None, SEQ, MP, None),
            P(),
            P(None, MP),
            P(None, MP),
            P(None, MP),
            P(),
            P(None, MP),
            P(MP),
            P(MP),
            P(MP),
            P(MP),
            P(MP, None),
            P(),
            P(SEQ, MP),
            P(MP, SEQ),
        ),
        out_specs=P(None, SEQ, MP, None),
        check_vma=False,
    )
```
